32 devices in a mesh: dp: 8 (over z, x), tensor: 4 (over y, core).
Axes of the slice: x: 2, y: 2, z: 4, core: 2. Of those that a mesh axis runs over, the one named last changes fastest.
Arguments:
- streams: bfloat16 [128, 4, 7168], P('dp', None, 'tensor'), may hold values from -12 to 12
- mix_weight: bfloat16 [24, 4, 7168], P(None, None, 'tensor'), may hold values from -0.0625 to 0.0625
- mix_bias: float32 [24], replicated, may hold values from -4 to 4
- gate_weight: bfloat16 [18432, 7168], P('dp', 'tensor'), may hold values from -0.0625 to 0.0625
- up_weight: bfloat16 [18432, 7168], P('dp', 'tensor'), may hold values from -0.0625 to 0.0625
- down_weight: bfloat16 [18432, 7168], P('dp', 'tensor'), may hold values from -0.046875 to 0.046875
Outputs:
- new_streams: bfloat16 [128, 4, 7168], P('dp', None, 'tensor')
The draws below stay inside these ranges and needn't reach their ends.
All inputs are finite; a program needn't handle non-finite values.
Results may differ from the reference program's by a relative error of at most 0.006.
The reference program's roundings to bfloat16 on the way (of `mlp_input` and `hidden`) count: a program that leaves them out, or rounds other values in their place, can miss the bound.
Values may be sent and summed in bfloat16 or wider, within the bound.
A program may use at most 64 MiB of HBM per device.

```python
import jax
import jax.numpy as jnp
from jax import lax

D = 7168
FF = 18432
STREAMS = 4
ITERS = 20
LOGITS = 24
TOKENS = 128


def draw_streams(key, part):
    normal_part = jax.random.normal(jax.random.fold_in(key, 11), (TOKENS, STREAMS, D), jnp.float32)
    return jnp.clip(normal_part, -12.0, 12.0).astype(jnp.bfloat16)


def block_scale(own_key, dims, split, low, high):
    level, own = 1.0, jax.random.fold_in(own_key, 6)
    for axis_at, shards_of in split:
        steps = jnp.exp(jax.random.uniform(jax.random.fold_in(own, axis_at), (shards_of,), jnp.float32, low / len(split), high / len(split)))
        level = level * jnp.repeat(steps, dims[axis_at] // shards_of).reshape([-1 if axis == axis_at else 1 for axis in range(len(dims))])
    return level


def gaussian(key, dims, width, limit, shards=(), held_as=jnp.bfloat16):
    entries = width * jax.random.normal(key, dims, jnp.float32)
    if shards:
        entries = entries * block_scale(key, dims, shards, -0.22, 0.18)
    return jnp.clip(entries, -limit, limit).astype(held_as)


def setup_inputs(seed: int = 0) -> dict:
    splits = jax.random.split(jax.random.key(seed), 7)
    streams = draw_streams(jax.random.fold_in(splits[6], 71), 0)
    mix_weight = gaussian(splits[1], (LOGITS, STREAMS, D), (2.0 / (STREAMS * D) ** 0.5), 0.0625, ((2, 4),))
    mix_bias = gaussian(splits[2], (LOGITS,), 1.0, 4.0, (), jnp.float32)
    gate_weight = gaussian(splits[3], (FF, D), D ** -0.5, 0.0625, ((0, 8), (1, 4)))
    up_weight = gaussian(splits[4], (FF, D), D ** -0.5, 0.0625, ((0, 8), (1, 4)))
    down_weight = gaussian(splits[5], (FF, D), FF ** -0.5, 0.046875, ((0, 8), (1, 4)))
    return {"streams": streams, "mix_weight": mix_weight, "mix_bias": mix_bias, "gate_weight": gate_weight, "up_weight": up_weight, "down_weight": down_weight}


epsilon = 1e-06

def normalize(sweep_index, matrix):
    matrix = matrix / lax.optimization_barrier(jnp.sum(matrix, axis=2, keepdims=True))
    return matrix / lax.optimization_barrier(jnp.sum(matrix, axis=1, keepdims=True))

def mixing(raw_logits, squares, mix_bias):
    scale_inv = lax.rsqrt(squares / (STREAMS * D) + epsilon)
    logits = raw_logits * scale_inv[:, None] + mix_bias[None, :]
    pre_gate = jax.nn.sigmoid(logits[:, :STREAMS])
    post_gate = 2.0 * jax.nn.sigmoid(logits[:, STREAMS:2 * STREAMS])
    matrix = jnp.exp(logits[:, 2 * STREAMS:]).reshape(-1, STREAMS, STREAMS)
    matrix = lax.fori_loop(0, ITERS, normalize, matrix)
    return (pre_gate, post_gate, matrix)

def reference(streams, mix_weight, mix_bias, gate_weight, up_weight, down_weight):
    row_count = streams.shape[0]
    flat_rows = streams.reshape(row_count, STREAMS * D)
    raw_logits = jnp.dot(flat_rows, mix_weight.reshape(LOGITS, STREAMS * D).T, preferred_element_type=jnp.float32)
    stream_wide = streams.astype(jnp.float32)
    squares = lax.optimization_barrier(jnp.sum(stream_wide * stream_wide, axis=(1, 2)))
    pre_gate, post_gate, res_mix = mixing(raw_logits, squares, mix_bias)
    mlp_input = jnp.einsum('ts,tsc->tc', pre_gate, stream_wide, precision=lax.Precision.HIGHEST).astype(jnp.bfloat16)
    gate = jnp.dot(mlp_input, gate_weight.T, preferred_element_type=jnp.float32)
    up_part = jnp.dot(mlp_input, up_weight.T, preferred_element_type=jnp.float32)
    hidden = (jax.nn.silu(gate) * up_part).astype(jnp.bfloat16)
    mlp_out = jnp.dot(hidden, down_weight, preferred_element_type=jnp.float32)
    mixed = jnp.einsum('tij,tjc->tic', res_mix, stream_wide, precision=lax.Precision.HIGHEST)
    mixed = mixed + post_gate[:, :, None] * mlp_out[:, None, :]
    return mixed.astype(jnp.bfloat16)
```

```python
import functools
import math

import jax
import jax.numpy as jnp
from jax import lax
from jax.experimental import pallas as pl
from jax.experimental.pallas import tpu as pltpu
from jax.sharding import PartitionSpec as P

D = 7168
ITERS = 20


epsilon = 1e-06


def normalize(sweep_index, matrix):
    matrix = matrix / jnp.sum(matrix, axis=2, keepdims=True)
    return matrix / jnp.sum(matrix, axis=1, keepdims=True)


def mixing(raw_logits, squares, mix_bias, stream_count):
    scale_inv = lax.rsqrt(squares / (stream_count * D) + epsilon)
    logits = raw_logits * scale_inv[:, None] + mix_bias[None, :]
    pre_gate = jax.nn.sigmoid(logits[:, :stream_count])
    post_gate = 2.0 * jax.nn.sigmoid(logits[:, stream_count : 2 * stream_count])
    matrix = jnp.exp(logits[:, 2 * stream_count :]).reshape(-1, stream_count, stream_count)
    matrix = lax.fori_loop(0, ITERS, normalize, matrix)
    return (pre_gate, post_gate, matrix)


def contract_last(weights, rows):
    return lax.dot_general(
        weights, rows, (((1,), (1,)), ((), ())), preferred_element_type=jnp.float32
    )


def per_device(streams, mix_weight, mix_bias, gate_weight, up_weight, down_weight):
    tok_rows, stream_count, width_local = streams.shape
    logit_count = mix_weight.shape[0]
    flat_rows = streams.reshape(tok_rows, stream_count * width_local)
    flat_weight = mix_weight.reshape(logit_count, stream_count * width_local)
    raw_logits = lax.dot_general(
        flat_rows, flat_weight, (((1,), (1,)), ((), ())), preferred_element_type=jnp.float32
    )
    stream_wide = streams.astype(jnp.float32)
    squares = jnp.sum(stream_wide * stream_wide, axis=(1, 2))
    total_logits, total_squares = lax.psum((raw_logits, squares), "tensor")
    pre_gate, post_gate, res_mix = mixing(total_logits, total_squares, mix_bias, stream_count)
    mlp_input = jnp.einsum(
        "ts,tsc->tc", pre_gate, stream_wide, precision=lax.Precision.HIGHEST
    ).astype(jnp.bfloat16)
    unit_local = gate_weight.shape[0]
    block_rows = lax.all_gather(mlp_input, "dp", axis=0, tiled=True)
    gate_part = contract_last(gate_weight, block_rows)
    up_part = contract_last(up_weight, block_rows)
    both_parts = jnp.concatenate((gate_part, up_part), axis=0)
    unit_share = lax.psum_scatter(both_parts, "tensor", scatter_dimension=1, tiled=True)
    hidden_share = (jax.nn.silu(unit_share[:unit_local]) * unit_share[unit_local:]).astype(
        jnp.bfloat16
    )
    hidden = lax.all_gather(hidden_share, "tensor", axis=1, tiled=True)
    mlp_out = lax.psum_scatter(
        lax.dot_general(
            hidden, down_weight, (((0,), (0,)), ((), ())), preferred_element_type=jnp.float32
        ),
        "dp",
        scatter_dimension=0,
        tiled=True,
    )
    mixed = jnp.einsum("tij,tjc->tic", res_mix, stream_wide, precision=lax.Precision.HIGHEST)
    mixed = mixed + post_gate[:, :, None] * mlp_out[:, None, :]
    return mixed.astype(jnp.bfloat16)


MESH = pl.DeviceIdType.MESH
UNIT_CHUNK = 256
COLUMN_CHUNK = 256
PAIR = 2
GROUP = 3
D_LAG = 4
VMEM_BUDGET = 58 * 1024 * 1024


def column(values, at):
    return values[:, at : at + 1]


def sigmoid(v):
    return 1.0 / (1.0 + jnp.exp(-v))


def layer_kernel(
    plan,
    s_hbm,
    mw_hbm,
    bias_ref,
    gate_hbm,
    up_hbm,
    down_hbm,
    out_hbm,
    out_ref,
    gate_v,
    up_v,
    down_v,
    s_raw,
    mw_raw,
    s_ref,
    mw_ref,
    part,
    part_in,
    post,
    rows_all,
    mixed,
    sums,
    pair_in,
    pair_sum,
    ring_out,
    ring_in,
    hidden,
    prod,
    cross_out,
    cross_in,
    cross_sum,
    line_out,
    line_in,
    entry,
    in_sem,
    w_sem,
    a_send,
    a_recv,
    bz_send,
    bz_recv,
    bx_send,
    bx_recv,
    c1_send,
    c1_recv,
    c2_send,
    c2_recv,
    c3_send,
    c3_recv,
    c4_send,
    c4_recv,
    d1_send,
    d1_recv,
    d2_send,
    d2_recv,
    out_sem,
):
    zs, ys, tensors, chunks, nc, columns, cc, width_all = plan
    streams, tok, width = s_ref.shape
    dp = lax.axis_index("dp")
    tp = lax.axis_index("tensor")
    z, x = lax.div(dp, PAIR), lax.rem(dp, PAIR)
    y, core = lax.div(tp, PAIR), lax.rem(tp, PAIR)
    x_peer = (z * PAIR + 1 - x, tp)
    core_peer = (dp, y * PAIR + 1 - core)

    def z_at(r):
        return lax.rem(z + r + zs, zs)

    def y_at(r):
        return lax.rem(y + r + ys, ys)

    def z_peer(r):
        return (z_at(r) * PAIR + x, tp)

    def y_peer(r):
        return (dp, y_at(r) * PAIR + core)

    def t_peer(r):
        return (dp, lax.rem(tp + r, tensors))

    def send(src, dst, ssem, rsem, peer):
        return pltpu.make_async_remote_copy(
            src_ref=src, dst_ref=dst, send_sem=ssem, recv_sem=rsem, device_id=peer, device_id_type=MESH
        )

    def weight_copy(k, which):
        hbm, vmem = ((gate_hbm, gate_v), (up_hbm, up_v), (down_hbm, down_v))[which]
        return pltpu.make_async_copy(hbm.at[pl.ds(k * nc, nc)], vmem.at[pl.ds(k * nc, nc)], w_sem.at[which])

    def weight_wait(which):
        hbm, vmem = ((gate_hbm, gate_v), (up_hbm, up_v), (down_hbm, down_v))[which]
        pltpu.make_async_copy(hbm, vmem, w_sem.at[which]).wait()

    def start_gate_up(k, _):
        weight_copy(k, 0).start()
        weight_copy(k, 1).start()
        return 0

    def start_down(k, _):
        weight_copy(k, 2).start()
        return 0

    barrier = pltpu.get_barrier_semaphore()
    peers = [t_peer(r) for r in range(1, tensors)] + [x_peer] + [z_peer(r) for r in range(1, zs)]
    for peer in peers:
        pl.semaphore_signal(barrier, inc=1, device_id=peer, device_id_type=MESH)

    inputs = (
        pltpu.make_async_copy(s_hbm, s_raw, in_sem.at[0]),
        pltpu.make_async_copy(mw_hbm, mw_raw, in_sem.at[1]),
    )
    for copy in inputs:
        copy.start()
    lax.fori_loop(0, chunks, start_gate_up, 0)
    lax.fori_loop(0, chunks, start_down, 0)
    for copy in inputs:
        copy.wait()
    for j in range(streams):
        s_ref[j] = s_raw[:, j, :]
        mw_ref[j] = mw_raw[:, j, :]

    raw = jnp.zeros((tok, mw_ref.shape[1]), jnp.float32)
    squares = jnp.zeros((tok, 1), jnp.float32)
    for j in range(streams):
        raw += contract_last(s_ref[j], mw_ref[j])
        wide = s_ref[j].astype(jnp.float32)
        squares += jnp.sum(wide * wide, axis=1, keepdims=True)
    count = raw.shape[1]
    part[...] = jnp.broadcast_to(squares, part.shape)
    part[:, :count] = raw
    pl.semaphore_wait(barrier, len(peers))

    def a_copy(r):
        return send(part, part_in.at[r - 1], a_send.at[0], a_recv.at[0], t_peer(r))

    def a_all():
        return send(part_in, part_in, a_send.at[0], a_recv.at[0], t_peer(1))

    for r in range(1, tensors):
        a_copy(r).start()
    a_all().wait_recv()
    total = part[...]
    for r in range(1, tensors):
        total = total + part_in[r - 1]
    scale_inv = lax.rsqrt(column(total, count) / width_all + epsilon)
    logits = total[:, :count] * scale_inv + bias_ref[...]
    gates = sigmoid(logits)
    mlp_input = column(gates, 0) * s_ref[0].astype(jnp.float32)
    for j in range(1, streams):
        mlp_input += column(gates, j) * s_ref[j].astype(jnp.float32)
    rows_all[z] = mlp_input.astype(jnp.bfloat16)

    def bz_copy(r):
        return send(rows_all.at[z], rows_all.at[z], bz_send.at[0], bz_recv.at[r - 1], z_peer(r))

    def bx_copy(r):
        at = z_at(-r)
        return send(rows_all.at[at], rows_all.at[zs + at], bx_send.at[0], bx_recv.at[0], x_peer)

    bx_copy(0).start()
    for r in range(1, zs):
        bz_copy(r).start()
    for i in range(streams):
        post[i] = jnp.broadcast_to(2.0 * column(gates, streams + i), (tok, post.shape[2]))

    order = sorted(range(1, zs), key=lambda r: min(r, zs - r))
    for r in order:
        send(rows_all.at[z], rows_all.at[z_at(-r)], bz_send.at[0], bz_recv.at[r - 1], z_peer(r)).wait_recv()
        bx_copy(r).start()

    entry[...] = jnp.zeros_like(entry)
    entry[:, :count] = jnp.exp(logits)
    turned = entry[...].T
    mat = tuple(turned[2 * streams + at : 2 * streams + at + 1] for at in range(streams * streams))

    def sweep(_, m):
        m = list(m)
        for i in range(streams):
            total_row = m[i * streams]
            for j in range(1, streams):
                total_row = total_row + m[i * streams + j]
            inv = 1.0 / total_row
            for j in range(streams):
                m[i * streams + j] = m[i * streams + j] * inv
        for j in range(streams):
            total_col = m[j]
            for i in range(1, streams):
                total_col = total_col + m[i * streams + j]
            inv = 1.0 / total_col
            for i in range(streams):
                m[i * streams + j] = m[i * streams + j] * inv
        return tuple(m)

    mat = lax.fori_loop(0, ITERS, sweep, mat)
    res = jnp.concatenate(mat + (jnp.zeros((128 - len(mat), tok), jnp.float32),), axis=0).T
    for i in range(streams):
        line = column(res, i * streams) * s_ref[0].astype(jnp.float32)
        for j in range(1, streams):
            line += column(res, i * streams + j) * s_ref[j].astype(jnp.float32)
        mixed[i] = line

    received = rows_all.at[pl.ds(zs, zs)]

    def bx_all():
        return send(received, received, bx_send.at[0], bx_recv.at[0], x_peer)

    bx_all().wait_recv()
    for which in range(3):
        weight_wait(which)

    prod[...] = jnp.zeros_like(prod)
    group = GROUP if chunks % GROUP == 0 else 1

    tokens = PAIR * zs * tok
    half = tokens // PAIR
    quarter = half // ys
    own_slot = core * ys + y

    def c1_copy(k):
        return send(sums.at[k, 1 - core], pair_in.at[k], c1_send.at[0], c1_recv.at[k], core_peer)

    def c2_copy(k, r):
        at = (k * (ys - 1)) + r - 1
        return send(ring_out.at[at], ring_in.at[at], c2_send.at[0], c2_recv.at[at], y_peer(r))

    def units(k):
        return pl.ds(pl.multiple_of(k * nc, nc), nc)

    def c3_copy(k, r):
        at = (k * (ys - 1)) + r - 1
        piece = hidden.at[own_slot, :, units(k)]
        return send(piece, piece, c3_send.at[0], c3_recv.at[at], y_peer(r))

    def c3_arrival(k, r):
        at = (k * (ys - 1)) + r - 1
        piece = hidden.at[core * ys + y_at(-r), :, units(k)]
        return send(piece, piece, c3_send.at[0], c3_recv.at[at], y_peer(r))

    def c4_copy(k, r):
        piece = hidden.at[core * ys + y_at(-r), :, units(k)]
        return send(piece, piece, c4_send.at[0], c4_recv.at[k], core_peer)

    def c4_arrival(k):
        piece = hidden.at[pl.ds((1 - core) * ys, ys), :, units(k)]
        return send(piece, piece, c4_send.at[0], c4_recv.at[k], core_peer)

    def c_first(k):
        rows = rows_all[...].reshape(tokens, width)
        sums[k, :, :, :nc] = contract_last(rows, gate_v[pl.ds(k * nc, nc)]).reshape(PAIR, half, nc)
        sums[k, :, :, nc:] = contract_last(rows, up_v[pl.ds(k * nc, nc)]).reshape(PAIR, half, nc)
        c1_copy(k).start()

    def c_second(k):
        c1_copy(k).wait_recv()
        both = sums[k, core] + pair_in[k]
        pair_sum[k] = both.reshape(ys, quarter, PAIR * nc)
        for r in range(1, ys):
            ring_out[k * (ys - 1) + r - 1] = pair_sum[k, y_at(r)].astype(jnp.bfloat16)
            c2_copy(k, r).start()

    def c_third(k):
        both = pair_sum[k, y]
        for r in range(1, ys):
            c2_copy(k, r).wait_recv()
            both = both + ring_in[k * (ys - 1) + r - 1].astype(jnp.float32)
        gate, up = both[:, :nc], both[:, nc:]
        hidden[own_slot, :, units(k)] = (gate / (1.0 + jnp.exp(-gate)) * up).astype(jnp.bfloat16)
        for r in range(1, ys):
            c3_copy(k, r).start()
        c4_copy(k, 0).start()

    def c_fourth(k):
        for r in range(1, ys):
            c3_arrival(k, r).wait_recv()
            c4_copy(k, r).start()

    def pipeline(count, stages):
        last = max(lag for lag, _ in stages)

        def step(t, _):
            for lag, stage in stages:
                @pl.when(jnp.logical_and(t >= lag, t < count + lag))
                def _():
                    stage(t - lag)

            return 0

        lax.fori_loop(0, count + last, step, 0)

    def cols(n):
        return pl.ds(pl.multiple_of(n * cc, cc), cc)

    def down_piece(first, n):
        span = pl.ds(pl.multiple_of(first * nc, nc), group * nc)
        rows = hidden[:, :, span].reshape(tokens, group * nc)
        return jnp.dot(rows, down_v[span, cols(n)], preferred_element_type=jnp.float32)

    def c_fifth(k):
        c4_arrival(k).wait_recv()

        @pl.when(jnp.logical_and(lax.rem(k, group) == group - 1, k < chunks - group))
        def _():
            def add(n, _):
                prod[n] = prod[n] + down_piece(k - (group - 1), n)
                return 0

            lax.fori_loop(0, columns, add, 0)

    pipeline(chunks, ((0, c_first), (2, c_second), (5, c_third), (8, c_fourth), (10, c_fifth)))

    def d1_copy(n):
        return send(cross_out.at[n], cross_in.at[n], d1_send.at[0], d1_recv.at[n], x_peer)

    def d2_copy(n, r):
        at = n * (zs - 1) + r - 1
        return send(line_out.at[at], line_in.at[at], d2_send.at[0], d2_recv.at[n], z_peer(r))

    def d2_arrival(n):
        piece = line_in.at[pl.ds(n * (zs - 1), zs - 1)]
        return send(piece, piece, d2_send.at[0], d2_recv.at[n], z_peer(1))

    def d_first(n):
        product = prod[n] + down_piece(chunks - group, n)
        prod[n, :half] = product[:half]
        cross_out[n] = product[half:].astype(jnp.bfloat16)
        d1_copy(n).start()

    def d_second(n):
        d1_copy(n).wait_recv()
        cross_sum[n] = (prod[n, :half] + cross_in[n].astype(jnp.float32)).reshape(zs, tok, cc)
        for r in range(1, zs):
            line_out[n * (zs - 1) + r - 1] = cross_sum[n, z_at(r)].astype(jnp.bfloat16)
            d2_copy(n, r).start()

    def d_third(n):
        mlp_out = cross_sum[n, z]
        d2_arrival(n).wait_recv()
        for r in range(1, zs):
            mlp_out = mlp_out + line_in[n * (zs - 1) + r - 1].astype(jnp.float32)
        for i in range(streams):
            out_ref[i, :, cols(n)] = (mixed[i, :, cols(n)] + column(post[i], 0) * mlp_out).astype(jnp.bfloat16)
        pltpu.make_async_copy(out_ref.at[:, :, cols(n)], out_hbm.at[:, :, cols(n)], out_sem.at[0]).start()

    pipeline(columns, ((0, d_first), (D_LAG, d_second), (2 * D_LAG, d_third)))

    a_all().wait_send()
    sent = rows_all.at[pl.ds(0, zs - 1)]
    send(sent, sent, bz_send.at[0], bz_recv.at[0], z_peer(1)).wait_send()
    bx_all().wait_send()
    whole = [
        (pair_in, c1_send),
        (ring_in, c2_send),
        (cross_in, d1_send),
        (line_in, d2_send),
    ]
    for ref, sem in whole:
        send(ref, ref, sem.at[0], sem.at[0], x_peer).wait_send()
    own = hidden.at[pl.ds(0, ys - 1)]
    send(own, own, c3_send.at[0], c3_send.at[0], x_peer).wait_send()
    both = hidden.at[pl.ds(0, ys)]
    send(both, both, c4_send.at[0], c4_send.at[0], x_peer).wait_send()
    pltpu.make_async_copy(out_ref, out_hbm, out_sem.at[0]).wait()


def layer_scratch(zs, ys, tensors, tok, streams, logits, width, units, nc, cc):
    tokens = PAIR * zs * tok
    half = tokens // PAIR
    quarter = half // ys
    chunks, columns = units // nc, width // cc
    f32, bf16 = jnp.float32, jnp.bfloat16
    lanes = 128
    arrays = [
        ((streams, tok, width), bf16),
        ((units, width), bf16),
        ((units, width), bf16),
        ((units, width), bf16),
        ((tok, streams, width), bf16),
        ((logits, streams, width), bf16),
        ((streams, tok, width), bf16),
        ((streams, logits, width), bf16),
        ((tok, lanes), f32),
        ((tensors - 1, tok, lanes), f32),
        ((streams, tok, lanes), f32),
        ((PAIR * zs, tok, width), bf16),
        ((streams, tok, width), f32),
        ((chunks, PAIR, half, 2 * nc), f32),
        ((chunks, half, 2 * nc), f32),
        ((chunks, ys, quarter, 2 * nc), f32),
        ((chunks * (ys - 1), quarter, 2 * nc), bf16),
        ((chunks * (ys - 1), quarter, 2 * nc), bf16),
        ((PAIR * ys, quarter, units), bf16),
        ((columns, tokens, cc), f32),
        ((columns, half, cc), bf16),
        ((columns, half, cc), bf16),
        ((columns, zs, tok, cc), f32),
        ((columns * (zs - 1), tok, cc), bf16),
        ((columns * (zs - 1), tok, cc), bf16),
        ((tok, lanes), f32),
    ]
    sems = [(2,), (3,)]
    for count in (1, zs - 1, 1, chunks, chunks * (ys - 1), chunks * (ys - 1), chunks, columns, columns):
        sems += [(1,), (count,)]
    sems.append((1,))
    size = sum(math.prod(shape) * jnp.dtype(kind).itemsize for shape, kind in arrays)
    return arrays, sems, size


def fused(mesh, streams, mix_weight, mix_bias, gate_weight, up_weight, down_weight):
    tok, stream_count, width = streams.shape
    units = gate_weight.shape[0]
    dps, tensors = mesh.shape["dp"], mesh.shape["tensor"]
    zs, ys = dps // PAIR, tensors // PAIR
    nc, cc = UNIT_CHUNK, COLUMN_CHUNK
    arrays, sems, _ = layer_scratch(zs, ys, tensors, tok, stream_count, mix_weight.shape[0], width, units, nc, cc)
    plan = (zs, ys, tensors, units // nc, nc, width // cc, cc, stream_count * width * tensors)
    bias = mix_bias[None, :]
    vmem = pl.BlockSpec(memory_space=pltpu.VMEM)
    hbm = pl.BlockSpec(memory_space=pl.ANY)
    out = pl.pallas_call(
        functools.partial(layer_kernel, plan),
        out_shape=jax.ShapeDtypeStruct((stream_count, tok, width), jnp.bfloat16),
        in_specs=[hbm, hbm, vmem, hbm, hbm, hbm],
        out_specs=hbm,
        scratch_shapes=[pltpu.VMEM(shape, kind) for shape, kind in arrays]
        + [pltpu.SemaphoreType.DMA(shape) for shape in sems],
        compiler_params=pltpu.CompilerParams(
            collective_id=0, has_side_effects=True, vmem_limit_bytes=VMEM_BUDGET
        ),
    )(streams, mix_weight, bias, gate_weight, up_weight, down_weight)
    return out.transpose(1, 0, 2)


def fits(mesh, streams, mix_weight, gate_weight):
    tok, stream_count, width = streams.shape
    units = gate_weight.shape[0]
    dps, tensors = mesh.shape["dp"], mesh.shape["tensor"]
    if dps % PAIR or tensors % PAIR or dps < 2 * PAIR or tensors < 2 * PAIR:
        return False
    zs, ys = dps // PAIR, tensors // PAIR
    if units % UNIT_CHUNK or width % COLUMN_CHUNK or tok % 16 or (zs * tok) % (16 * ys):
        return False
    if mix_weight.shape[0] >= 128:
        return False
    size = layer_scratch(
        zs, ys, tensors, tok, stream_count, mix_weight.shape[0], width, units, UNIT_CHUNK, COLUMN_CHUNK
    )[2]
    return size < VMEM_BUDGET * 3 // 4


def solution(mesh):
    in_specs = (
        P("dp", None, "tensor"),
        P(None, None, "tensor"),
        P(),
        P("dp", "tensor"),
        P("dp", "tensor"),
        P("dp", "tensor"),
    )
    out_specs = P("dp", None, "tensor")

    def step(streams, mix_weight, mix_bias, gate_weight, up_weight, down_weight):
        operands = (streams, mix_weight, mix_bias, gate_weight, up_weight, down_weight)
        if fits(mesh, streams, mix_weight, gate_weight):
            return fused(mesh, *operands)
        return per_device(*operands)

    return jax.shard_map(step, mesh=mesh, in_specs=in_specs, out_specs=out_specs, check_vma=False)
```

```python
import functools
import math

import jax
import jax.numpy as jnp
from jax import lax
from jax.experimental import pallas as pl
from jax.experimental.pallas import tpu as pltpu
from jax.sharding import PartitionSpec as P

D = 7168
ITERS = 20


epsilon = 1e-06


def normalize(sweep_index, matrix):
    matrix = matrix / jnp.sum(matrix, axis=2, keepdims=True)
    return matrix / jnp.sum(matrix, axis=1, keepdims=True)


def mixing(raw_logits, squares, mix_bias, stream_count):
    scale_inv = lax.rsqrt(squares / (stream_count * D) + epsilon)
    logits = raw_logits * scale_inv[:, None] + mix_bias[None, :]
    pre_gate = jax.nn.sigmoid(logits[:, :stream_count])
    post_gate = 2.0 * jax.nn.sigmoid(logits[:, stream_count : 2 * stream_count])
    matrix = jnp.exp(logits[:, 2 * stream_count :]).reshape(-1, stream_count, stream_count)
    matrix = lax.fori_loop(0, ITERS, normalize, matrix)
    return (pre_gate, post_gate, matrix)


def contract_last(weights, rows):
    return lax.dot_general(
        weights, rows, (((1,), (1,)), ((), ())), preferred_element_type=jnp.float32
    )


def per_device(streams, mix_weight, mix_bias, gate_weight, up_weight, down_weight):
    tok_rows, stream_count, width_local = streams.shape
    logit_count = mix_weight.shape[0]
    flat_rows = streams.reshape(tok_rows, stream_count * width_local)
    flat_weight = mix_weight.reshape(logit_count, stream_count * width_local)
    raw_logits = lax.dot_general(
        flat_rows, flat_weight, (((1,), (1,)), ((), ())), preferred_element_type=jnp.float32
    )
    stream_wide = streams.astype(jnp.float32)
    squares = jnp.sum(stream_wide * stream_wide, axis=(1, 2))
    total_logits, total_squares = lax.psum((raw_logits, squares), "tensor")
    pre_gate, post_gate, res_mix = mixing(total_logits, total_squares, mix_bias, stream_count)
    mlp_input = jnp.einsum(
        "ts,tsc->tc", pre_gate, stream_wide, precision=lax.Precision.HIGHEST
    ).astype(jnp.bfloat16)
    unit_local = gate_weight.shape[0]
    block_rows = lax.all_gather(mlp_input, "dp", axis=0, tiled=True)
    gate_part = contract_last(gate_weight, block_rows)
    up_part = contract_last(up_weight, block_rows)
    both_parts = jnp.concatenate((gate_part, up_part), axis=0)
    unit_share = lax.psum_scatter(both_parts, "tensor", scatter_dimension=1, tiled=True)
    hidden_share = (jax.nn.silu(unit_share[:unit_local]) * unit_share[unit_local:]).astype(
        jnp.bfloat16
    )
    hidden = lax.all_gather(hidden_share, "tensor", axis=1, tiled=True)
    mlp_out = lax.psum_scatter(
        lax.dot_general(
            hidden, down_weight, (((0,), (0,)), ((), ())), preferred_element_type=jnp.float32
        ),
        "dp",
        scatter_dimension=0,
        tiled=True,
    )
    mixed = jnp.einsum("tij,tjc->tic", res_mix, stream_wide, precision=lax.Precision.HIGHEST)
    mixed = mixed + post_gate[:, :, None] * mlp_out[:, None, :]
    return mixed.astype(jnp.bfloat16)


MESH = pl.DeviceIdType.MESH
UNIT_CHUNK = 256
COLUMN_CHUNK = 256
PAIR = 2
GROUPS = 2
LANES = 128
LAG_SUM = (3, 4)
LAG_HIDDEN = (8, 12)
LAG_FORWARD = 14
LATE = 4
LAG_CROSS = 7
LAG_OUT = 21
TURNS = (6, 4, 4)
VMEM_BUDGET = 58 * 1024 * 1024


def column(values, at):
    return values[:, at : at + 1]


def sigmoid(v):
    return 1.0 / (1.0 + jnp.exp(-v))


def sweep(count, _, entries):
    m = list(entries)
    for i in range(count):
        total_row = m[i * count]
        for j in range(1, count):
            total_row = total_row + m[i * count + j]
        inv = 1.0 / total_row
        for j in range(count):
            m[i * count + j] = m[i * count + j] * inv
    for j in range(count):
        total_col = m[j]
        for i in range(1, count):
            total_col = total_col + m[i * count + j]
        inv = 1.0 / total_col
        for i in range(count):
            m[i * count + j] = m[i * count + j] * inv
    return tuple(m)


def layer_kernel(
    plan,
    s_hbm,
    mw_hbm,
    bias_ref,
    gate_hbm,
    up_hbm,
    down_hbm,
    out_hbm,
    out_ref,
    gate_v,
    up_v,
    down_v,
    s_raw,
    mw_raw,
    s_ref,
    mw_ref,
    part,
    part_in,
    entry,
    post,
    rows_all,
    mixed,
    sums,
    pair_in,
    ring_out,
    ring_in,
    hidden,
    own,
    cross_out,
    cross_in,
    cross_sum,
    line_out,
    line_in,
    in_sem,
    w_sem,
    out_sem,
    a_send,
    a_recv,
    bz_send,
    bz_recv,
    bx_send,
    bx_recv,
    c1_send,
    c1_recv,
    c2_send,
    c2_recv,
    c3_send,
    c3_recv,
    c4_send,
    c4_recv,
    d1_send,
    d1_recv,
    d2_send,
    d2_recv,
):
    zs, ys, tensors, chunks, nc, columns, cc, width_all = plan
    streams, tok, width = s_ref.shape
    scope = jax.named_scope
    dp = lax.axis_index("dp")
    tp = lax.axis_index("tensor")
    z, x = lax.div(dp, PAIR), lax.rem(dp, PAIR)
    y, core = lax.div(tp, PAIR), lax.rem(tp, PAIR)
    x_peer = (z * PAIR + 1 - x, tp)
    core_peer = (dp, y * PAIR + 1 - core)
    zb = zs // GROUPS
    gh = zb * tok
    gq = gh // ys
    z_half, z_odd = lax.div(z, zb), lax.rem(z, zb)
    own_group = lax.rem(lax.div(z + 1, zb), GROUPS)

    def slot_of(at):
        return lax.rem(lax.div(at + 1, zb), GROUPS) * zb + lax.div(at, zb)

    def y_at(r):
        return lax.rem(y + r + ys, ys)

    def z_dev(at):
        return (at * PAIR + x, tp)

    def z_peer(r):
        return z_dev(lax.rem(z + r + zs, zs))

    def y_peer(r):
        return (dp, y_at(r) * PAIR + core)

    def t_peer(r):
        return (dp, lax.rem(tp + r, tensors))

    def send(src, dst, ssem, rsem, peer):
        return pltpu.make_async_remote_copy(
            src_ref=src, dst_ref=dst, send_sem=ssem, recv_sem=rsem, device_id=peer, device_id_type=MESH
        )

    weights = ((gate_hbm, gate_v), (up_hbm, up_v), (down_hbm, down_v))

    def start_weights(k, _, which):
        hbm, vmem = weights[which]
        part_of = pl.ds(k * nc, nc)
        pltpu.make_async_copy(hbm.at[part_of], vmem.at[part_of], w_sem.at[which]).start()
        return 0

    def weight_wait(which):
        hbm, vmem = weights[which]
        pltpu.make_async_copy(hbm, vmem, w_sem.at[which]).wait()

    barrier = pltpu.get_barrier_semaphore()
    peers = [t_peer(r) for r in range(1, tensors)] + [x_peer] + [z_peer(r) for r in range(1, zs)]
    with scope("start"):
        for peer in peers:
            pl.semaphore_signal(barrier, inc=1, device_id=peer, device_id_type=MESH)
        inputs = (
            pltpu.make_async_copy(s_hbm, s_raw, in_sem.at[0]),
            pltpu.make_async_copy(mw_hbm, mw_raw, in_sem.at[1]),
        )
        for copy in inputs:
            copy.start()
        for which in range(3):
            lax.fori_loop(0, chunks, functools.partial(start_weights, which=which), 0)
        for copy in inputs:
            copy.wait()
    with scope("relayout"):
        for j in range(streams):
            s_ref[j] = s_raw[:, j, :]
            mw_ref[j] = mw_raw[:, j, :]

    with scope("raw_logits"):
        raw = jnp.zeros((tok, mw_ref.shape[1]), jnp.float32)
        squares = jnp.zeros((tok, 1), jnp.float32)
        for j in range(streams):
            raw += contract_last(s_ref[j], mw_ref[j])
            wide = s_ref[j].astype(jnp.float32)
            squares += jnp.sum(wide * wide, axis=1, keepdims=True)
        count = raw.shape[1]
        part[...] = jnp.broadcast_to(squares, part.shape)
        part[:, :count] = raw
    with scope("barrier"):
        pl.semaphore_wait(barrier, len(peers))

    def a_copy(r):
        return send(part, part_in.at[r - 1], a_send.at[0], a_recv.at[0], t_peer(r))

    def a_all():
        return send(part_in, part_in, a_send.at[0], a_recv.at[0], t_peer(1))

    with scope("a_exchange"):
        for r in range(1, tensors):
            a_copy(r).start()
        a_all().wait_recv()
    with scope("gates"):
        total = part[...]
        for r in range(1, tensors):
            total = total + part_in[r - 1]
        scale_inv = lax.rsqrt(column(total, count) / width_all + epsilon)
        logits = total[:, :count] * scale_inv + bias_ref[...]
        gates = sigmoid(logits)
        mlp_input = column(gates, 0) * s_ref[0].astype(jnp.float32)
        for j in range(1, streams):
            mlp_input += column(gates, j) * s_ref[j].astype(jnp.float32)
        rows_all[slot_of(z)] = mlp_input.astype(jnp.bfloat16)

    mate, inner, outer = z_half * zb + 1 - z_odd, zb - z_half, (zs - 1) * (1 - z_half)

    def bz_copy(source, target):
        block = rows_all.at[slot_of(source)]
        return send(block, block, bz_send.at[0], bz_recv.at[source], z_dev(target))

    def bx_copy(source):
        at = slot_of(source)
        return send(rows_all.at[at], rows_all.at[zs + at], bx_send.at[0], bx_recv.at[0], x_peer)

    def bx_all():
        received = rows_all.at[pl.ds(zs, zs)]
        return send(received, received, bx_send.at[0], bx_recv.at[0], x_peer)

    with scope("b_start"):
        for target in (mate, outer, inner):
            bz_copy(z, target).start()
        bx_copy(z).start()
        for i in range(streams):
            post[i] = jnp.broadcast_to(2.0 * column(gates, streams + i), (tok, post.shape[2]))
    def turn(k, _, which):
        with scope("turn"):
            vmem = weights[which][1]
            span = pl.ds(pl.multiple_of(k * nc, nc), nc)
            for at in range(0, width, nc):
                vmem[span, at : at + nc] = vmem[span, at : at + nc].T
        return 0

    def turns(first, last):
        for which in range(2):
            low, high = (min(max(at - which * chunks, 0), chunks) for at in (first, last))
            if low < high:
                lax.fori_loop(low, high, functools.partial(turn, which=which), 0)

    weight_wait(0)
    turned = 0
    for at, source in enumerate((mate, inner, outer)):
        if at == 1:
            weight_wait(1)
        turns(turned, turned + TURNS[at])
        turned += TURNS[at]
        with scope(f"b_forward{at}"):
            bz_copy(source, source).wait_recv()
            bx_copy(source).start()
    turns(turned, 2 * chunks)

    with scope("sinkhorn"):
        entry[...] = jnp.zeros_like(entry)
        entry[:, :count] = jnp.exp(logits)
        flipped = entry[...].T
        first = 2 * streams
        mat = tuple(flipped[first + at : first + at + 1] for at in range(streams * streams))
        mat = lax.fori_loop(0, ITERS, functools.partial(sweep, streams), mat)
    with scope("mixed"):
        rest = jnp.zeros((LANES - len(mat), tok), jnp.float32)
        res = jnp.concatenate(mat + (rest,), axis=0).T
        for i in range(streams):
            line = column(res, i * streams) * s_ref[0].astype(jnp.float32)
            for j in range(1, streams):
                line += column(res, i * streams + j) * s_ref[j].astype(jnp.float32)
            mixed[i] = line
    with scope("b_wait"):
        bx_all().wait_recv()
        weight_wait(2)

    own_slot = core * ys + y

    def c1_copy(k):
        return send(sums.at[k, 1 - core], pair_in.at[k], c1_send.at[0], c1_recv.at[k], core_peer)

    def c2_copy(k, g, r):
        at = k * GROUPS + g
        return send(ring_out.at[at, r - 1], ring_in.at[at, r - 1], c2_send.at[0], c2_recv.at[at], y_peer(r))

    def c2_arrival(k, g):
        piece = ring_in.at[k * GROUPS + g]
        return send(piece, piece, c2_send.at[0], c2_recv.at[k * GROUPS + g], y_peer(1))

    def units(k):
        return pl.ds(pl.multiple_of(k * nc, nc), nc)

    def quarter(at):
        return pl.ds(pl.multiple_of(at * gq, gq), gq)

    def c3_copy(k, g, r, source):
        at = (k * GROUPS + g) * (ys - 1) + r - 1
        piece = hidden.at[g, core * ys + source, :, units(k)]
        return send(piece, piece, c3_send.at[0], c3_recv.at[at], y_peer(r))

    def c4_copy(k, g, source):
        piece = hidden.at[g, core * ys + source, :, units(k)]
        return send(piece, piece, c4_send.at[0], c4_recv.at[g], core_peer)

    def c4_arrival(g):
        piece = hidden.at[g, pl.ds((1 - core) * ys, ys)]
        return send(piece, piece, c4_send.at[0], c4_recv.at[g], core_peer)

    def c_first(k):
        with scope("c_first"):
            rows = rows_all[...].reshape(PAIR * zs * tok, width)
            shape = (PAIR, GROUPS, gh, nc)
            for at, vmem in ((pl.ds(0, nc), gate_v), (pl.ds(nc, nc), up_v)):
                product = None
                for kt in range(0, width, nc):
                    term = jnp.dot(rows[:, kt : kt + nc], vmem[pl.ds(k * nc, nc), kt : kt + nc], preferred_element_type=jnp.float32)
                    product = term if product is None else product + term
                sums[k, :, :, :, at] = product.reshape(shape)
            c1_copy(k).start()

    def c_second(g, k):
        with scope(f"c_second{g}"):
            if g == 0:
                c1_copy(k).wait_recv()
            for r in range(1, ys):
                at = quarter(y_at(r))
                both = sums[k, core, g, at] + pair_in[k, g, at]
                ring_out[k * GROUPS + g, r - 1] = both.astype(jnp.bfloat16)
                c2_copy(k, g, r).start()

    def c_third(g, k):
        with scope(f"c_third{g}"):
            at = quarter(y)
            both = sums[k, core, g, at] + pair_in[k, g, at]
            c2_arrival(k, g).wait_recv()
            for r in range(1, ys):
                both = both + ring_in[k * GROUPS + g, r - 1].astype(jnp.float32)
            gate, up = both[:, :nc], both[:, nc:]
            hidden[g, own_slot, :, units(k)] = (gate / (1.0 + jnp.exp(-gate)) * up).astype(jnp.bfloat16)
            for r in range(1, ys):
                c3_copy(k, g, r, y).start()
            c4_copy(k, g, y).start()

    def c_fourth(g, k):
        with scope(f"c_fourth{g}"):
            for r in range(1, ys):
                c3_copy(k, g, r, y_at(-r)).wait_recv()
                c4_copy(k, g, y_at(-r)).start()

    def pipeline(steps, stages):
        def step(t, _):
            for lag, count, stage in stages:
                @pl.when(jnp.logical_and(t >= lag, t < count + lag))
                def _():
                    stage(t - lag)

            return 0

        lax.fori_loop(0, steps, step, 0)

    late = min(LATE, chunks)
    second, third, fourth = (
        [functools.partial(stage, g) for g in range(GROUPS)] for stage in (c_second, c_third, c_fourth)
    )
    pipeline(
        chunks + LAG_FORWARD,
        (
            (0, chunks, c_first),
            (LAG_SUM[0], chunks, second[0]),
            (LAG_SUM[1], chunks, second[1]),
            (LAG_HIDDEN[0], chunks, third[0]),
            (LAG_HIDDEN[1], chunks, third[1]),
            (LAG_FORWARD, chunks, fourth[0]),
            (LAG_FORWARD + late, chunks - late, fourth[1]),
        ),
    )

    def cols(n):
        return pl.ds(pl.multiple_of(n * cc, cc), cc)

    def d1_copy(job):
        return send(cross_out.at[job], cross_in.at[job], d1_send.at[0], d1_recv.at[job], x_peer)

    def d2_copy(job, n, b, r):
        return send(line_out.at[job, b], line_in.at[n, r - 1], d2_send.at[0], d2_recv.at[n], z_peer(r))

    def d2_arrival(n):
        return send(line_in.at[n], line_in.at[n], d2_send.at[0], d2_recv.at[n], z_peer(1))

    def d_first(job):
        g, n = lax.div(job, columns), lax.rem(job, columns)

        @pl.when(n == 0)
        def _():
            with scope("c4_wait"):
                c4_arrival(g).wait_recv()

        with scope("d_first"):
            rows = hidden[g].reshape(PAIR * gh, chunks * nc)
            product = jnp.dot(rows, down_v[:, cols(n)], preferred_element_type=jnp.float32)
            own[job] = product[:gh]
            cross_out[job] = product[gh:].astype(jnp.bfloat16)
            d1_copy(job).start()

    def d_second(job):
        g, n = lax.div(job, columns), lax.rem(job, columns)
        with scope("d_second"):
            d1_copy(job).wait_recv()
            summed = (own[job] + cross_in[job].astype(jnp.float32)).reshape(zb, tok, cc)
            cross_sum[job] = summed
            line_out[job] = summed.astype(jnp.bfloat16)
            for b in range(zb):
                r = lax.rem(zb * b + lax.rem(b + g, GROUPS) - z + zs, zs)

                @pl.when(r > 0)
                def _():
                    d2_copy(job, n, b, r).start()

    def d_third(job):
        g, n = lax.div(job, columns), lax.rem(job, columns)

        @pl.when(g == own_group)
        def _():
            with scope("d_third"):
                mlp_out = cross_sum[job, z_half]
                d2_arrival(n).wait_recv()
                for r in range(1, zs):
                    mlp_out = mlp_out + line_in[n, r - 1].astype(jnp.float32)
                for i in range(streams):
                    value = mixed[i, :, cols(n)] + column(post[i], 0) * mlp_out
                    out_ref[i, :, cols(n)] = value.astype(jnp.bfloat16)
                pltpu.make_async_copy(out_ref.at[:, :, cols(n)], out_hbm.at[:, :, cols(n)], out_sem.at[0]).start()

    jobs = GROUPS * columns
    pipeline(
        jobs + LAG_OUT,
        (
            (LAG_CROSS, jobs, d_second),
            (0, jobs, d_first),
            (1, late, lambda k: c_fourth(1, k + chunks - late)),
            (LAG_OUT, jobs, d_third),
        ),
    )

    with scope("drain"):
        a_all().wait_send()
        bx_all().wait_send()
        whole = [
            (rows_all.at[pl.ds(0, zs - 1)], bz_send),
            (pair_in, c1_send),
            (ring_in, c2_send),
            (hidden.at[:, pl.ds(0, ys - 1)], c3_send),
            (hidden.at[:, pl.ds(0, ys)], c4_send),
            (cross_in, d1_send),
            (line_in, d2_send),
        ]
        for ref, sem in whole:
            send(ref, ref, sem.at[0], sem.at[0], x_peer).wait_send()
        pltpu.make_async_copy(out_ref, out_hbm, out_sem.at[0]).wait()


def layer_scratch(zs, ys, tensors, tok, streams, logits, width, units, nc, cc):
    zb = zs // GROUPS
    gh = zb * tok
    gq = gh // ys
    chunks, columns = units // nc, width // cc
    jobs = GROUPS * columns
    f32, bf16 = jnp.float32, jnp.bfloat16
    arrays = [
        ((streams, tok, width), bf16),
        ((units, width), bf16),
        ((units, width), bf16),
        ((units, width), bf16),
        ((tok, streams, width), bf16),
        ((logits, streams, width), bf16),
        ((streams, tok, width), bf16),
        ((streams, logits, width), bf16),
        ((tok, LANES), f32),
        ((tensors - 1, tok, LANES), f32),
        ((tok, LANES), f32),
        ((streams, tok, LANES), f32),
        ((PAIR * zs, tok, width), bf16),
        ((streams, tok, width), f32),
        ((chunks, PAIR, GROUPS, gh, 2 * nc), f32),
        ((chunks, GROUPS, gh, 2 * nc), f32),
        ((chunks * GROUPS, ys - 1, gq, 2 * nc), bf16),
        ((chunks * GROUPS, ys - 1, gq, 2 * nc), bf16),
        ((GROUPS, PAIR * ys, gq, units), bf16),
        ((jobs, gh, cc), f32),
        ((jobs, gh, cc), bf16),
        ((jobs, gh, cc), bf16),
        ((jobs, zb, tok, cc), f32),
        ((jobs, zb, tok, cc), bf16),
        ((columns, zs - 1, tok, cc), bf16),
    ]
    sems = [(2,), (3,), (1,)]
    for count in (1, zs, 1, chunks, chunks * GROUPS, chunks * GROUPS * (ys - 1), GROUPS, jobs, columns):
        sems += [(1,), (count,)]
    size = sum(math.prod(shape) * jnp.dtype(kind).itemsize for shape, kind in arrays)
    return arrays, sems, size


def fused(mesh, streams, mix_weight, mix_bias, gate_weight, up_weight, down_weight):
    tok, stream_count, width = streams.shape
    units = gate_weight.shape[0]
    dps, tensors = mesh.shape["dp"], mesh.shape["tensor"]
    zs, ys = dps // PAIR, tensors // PAIR
    nc, cc = UNIT_CHUNK, COLUMN_CHUNK
    arrays, sems, _ = layer_scratch(zs, ys, tensors, tok, stream_count, mix_weight.shape[0], width, units, nc, cc)
    plan = (zs, ys, tensors, units // nc, nc, width // cc, cc, stream_count * width * tensors)
    bias = mix_bias[None, :]
    vmem = pl.BlockSpec(memory_space=pltpu.VMEM)
    hbm = pl.BlockSpec(memory_space=pl.ANY)
    out = pl.pallas_call(
        functools.partial(layer_kernel, plan),
        out_shape=jax.ShapeDtypeStruct((stream_count, tok, width), jnp.bfloat16),
        in_specs=[hbm, hbm, vmem, hbm, hbm, hbm],
        out_specs=hbm,
        scratch_shapes=[pltpu.VMEM(shape, kind) for shape, kind in arrays]
        + [pltpu.SemaphoreType.DMA(shape) for shape in sems],
        compiler_params=pltpu.CompilerParams(
            collective_id=0, has_side_effects=True, vmem_limit_bytes=VMEM_BUDGET
        ),
    )(streams, mix_weight, bias, gate_weight, up_weight, down_weight)
    return out.transpose(1, 0, 2)


def fits(mesh, streams, mix_weight, gate_weight):
    tok, stream_count, width = streams.shape
    units = gate_weight.shape[0]
    dps, tensors = mesh.shape["dp"], mesh.shape["tensor"]
    if dps != PAIR * GROUPS * PAIR or tensors % PAIR or tensors < 2 * PAIR:
        return False
    zs, ys = dps // PAIR, tensors // PAIR
    if units % UNIT_CHUNK or width % COLUMN_CHUNK or tok % 16 or (zs // GROUPS * tok) % (16 * ys):
        return False
    if mix_weight.shape[0] >= LANES:
        return False
    size = layer_scratch(
        zs, ys, tensors, tok, stream_count, mix_weight.shape[0], width, units, UNIT_CHUNK, COLUMN_CHUNK
    )[2]
    return size < VMEM_BUDGET * 3 // 4


def solution(mesh):
    in_specs = (
        P("dp", None, "tensor"),
        P(None, None, "tensor"),
        P(),
        P("dp", "tensor"),
        P("dp", "tensor"),
        P("dp", "tensor"),
    )
    out_specs = P("dp", None, "tensor")

    def step(streams, mix_weight, mix_bias, gate_weight, up_weight, down_weight):
        operands = (streams, mix_weight, mix_bias, gate_weight, up_weight, down_weight)
        if fits(mesh, streams, mix_weight, gate_weight):
            return fused(mesh, *operands)
        return per_device(*operands)

    return jax.shard_map(step, mesh=mesh, in_specs=in_specs, out_specs=out_specs, check_vma=False)
```

```python
import functools
import math

import jax
import jax.numpy as jnp
from jax import lax
from jax.experimental import pallas as pl
from jax.experimental.pallas import tpu as pltpu
from jax.sharding import PartitionSpec as P

D = 7168
ITERS = 20


epsilon = 1e-06


def normalize(sweep_index, matrix):
    matrix = matrix / jnp.sum(matrix, axis=2, keepdims=True)
    return matrix / jnp.sum(matrix, axis=1, keepdims=True)


def mixing(raw_logits, squares, mix_bias, stream_count):
    scale_inv = lax.rsqrt(squares / (stream_count * D) + epsilon)
    logits = raw_logits * scale_inv[:, None] + mix_bias[None, :]
    pre_gate = jax.nn.sigmoid(logits[:, :stream_count])
    post_gate = 2.0 * jax.nn.sigmoid(logits[:, stream_count : 2 * stream_count])
    matrix = jnp.exp(logits[:, 2 * stream_count :]).reshape(-1, stream_count, stream_count)
    matrix = lax.fori_loop(0, ITERS, normalize, matrix)
    return (pre_gate, post_gate, matrix)


def contract_last(weights, rows):
    return lax.dot_general(
        weights, rows, (((1,), (1,)), ((), ())), preferred_element_type=jnp.float32
    )


def per_device(streams, mix_weight, mix_bias, gate_weight, up_weight, down_weight):
    tok_rows, stream_count, width_local = streams.shape
    logit_count = mix_weight.shape[0]
    flat_rows = streams.reshape(tok_rows, stream_count * width_local)
    flat_weight = mix_weight.reshape(logit_count, stream_count * width_local)
    raw_logits = lax.dot_general(
        flat_rows, flat_weight, (((1,), (1,)), ((), ())), preferred_element_type=jnp.float32
    )
    stream_wide = streams.astype(jnp.float32)
    squares = jnp.sum(stream_wide * stream_wide, axis=(1, 2))
    total_logits, total_squares = lax.psum((raw_logits, squares), "tensor")
    pre_gate, post_gate, res_mix = mixing(total_logits, total_squares, mix_bias, stream_count)
    mlp_input = jnp.einsum(
        "ts,tsc->tc", pre_gate, stream_wide, precision=lax.Precision.HIGHEST
    ).astype(jnp.bfloat16)
    unit_local = gate_weight.shape[0]
    block_rows = lax.all_gather(mlp_input, "dp", axis=0, tiled=True)
    gate_part = contract_last(gate_weight, block_rows)
    up_part = contract_last(up_weight, block_rows)
    both_parts = jnp.concatenate((gate_part, up_part), axis=0)
    unit_share = lax.psum_scatter(both_parts, "tensor", scatter_dimension=1, tiled=True)
    hidden_share = (jax.nn.silu(unit_share[:unit_local]) * unit_share[unit_local:]).astype(
        jnp.bfloat16
    )
    hidden = lax.all_gather(hidden_share, "tensor", axis=1, tiled=True)
    mlp_out = lax.psum_scatter(
        lax.dot_general(
            hidden, down_weight, (((0,), (0,)), ((), ())), preferred_element_type=jnp.float32
        ),
        "dp",
        scatter_dimension=0,
        tiled=True,
    )
    mixed = jnp.einsum("tij,tjc->tic", res_mix, stream_wide, precision=lax.Precision.HIGHEST)
    mixed = mixed + post_gate[:, :, None] * mlp_out[:, None, :]
    return mixed.astype(jnp.bfloat16)


MESH = pl.DeviceIdType.MESH
UNIT_CHUNK = 256
COLUMN_CHUNK = 256
PAIR = 2
GROUPS = 2
LANES = 128
LAG_SUM = (3, 4)
LAG_HIDDEN = (8, 12)
LAG_FORWARD = 14
LATE = 4
LAG_CROSS = 7
LAG_OUT = 21
TURNS = (8, 3, 2)
VMEM_BUDGET = 58 * 1024 * 1024


def column(values, at):
    return values[:, at : at + 1]


def sigmoid(v):
    return 1.0 / (1.0 + jnp.exp(-v))


def sweep(count, _, entries):
    m = list(entries)
    for i in range(count):
        total_row = m[i * count]
        for j in range(1, count):
            total_row = total_row + m[i * count + j]
        inv = 1.0 / total_row
        for j in range(count):
            m[i * count + j] = m[i * count + j] * inv
    for j in range(count):
        total_col = m[j]
        for i in range(1, count):
            total_col = total_col + m[i * count + j]
        inv = 1.0 / total_col
        for i in range(count):
            m[i * count + j] = m[i * count + j] * inv
    return tuple(m)


def layer_kernel(
    plan,
    s_hbm,
    mw_hbm,
    bias_ref,
    gate_hbm,
    up_hbm,
    down_hbm,
    out_ref,
    gate_v,
    up_v,
    down_v,
    s_raw,
    mw_raw,
    s_ref,
    mw_ref,
    part,
    part_in,
    entry,
    post,
    rows_all,
    mixed,
    sums,
    pair_in,
    ring_out,
    ring_in,
    hidden,
    own,
    cross_out,
    cross_in,
    cross_sum,
    line_out,
    line_in,
    in_sem,
    w_sem,
    a_send,
    a_recv,
    bz_send,
    bz_recv,
    bx_send,
    bx_recv,
    c1_send,
    c1_recv,
    c2_send,
    c2_recv,
    c3_send,
    c3_recv,
    c4_send,
    c4_recv,
    d1_send,
    d1_recv,
    d2_send,
    d2_recv,
):
    zs, ys, tensors, chunks, nc, columns, cc, width_all = plan
    streams, tok, width = s_ref.shape
    scope = jax.named_scope
    dp = lax.axis_index("dp")
    tp = lax.axis_index("tensor")
    z, x = lax.div(dp, PAIR), lax.rem(dp, PAIR)
    y, core = lax.div(tp, PAIR), lax.rem(tp, PAIR)
    x_peer = (z * PAIR + 1 - x, tp)
    core_peer = (dp, y * PAIR + 1 - core)
    zb = zs // GROUPS
    gh = zb * tok
    gq = gh // ys
    z_half, z_odd = lax.div(z, zb), lax.rem(z, zb)
    own_group = lax.rem(lax.div(z + 1, zb), GROUPS)

    def slot_of(at):
        return lax.rem(lax.div(at + 1, zb), GROUPS) * zb + lax.div(at, zb)

    def y_at(r):
        return lax.rem(y + r + ys, ys)

    def z_dev(at):
        return (at * PAIR + x, tp)

    def z_peer(r):
        return z_dev(lax.rem(z + r + zs, zs))

    def y_peer(r):
        return (dp, y_at(r) * PAIR + core)

    def t_peer(r):
        return (dp, lax.rem(tp + r, tensors))

    def send(src, dst, ssem, rsem, peer):
        return pltpu.make_async_remote_copy(
            src_ref=src, dst_ref=dst, send_sem=ssem, recv_sem=rsem, device_id=peer, device_id_type=MESH
        )

    weights = ((gate_hbm, gate_v), (up_hbm, up_v), (down_hbm, down_v))

    def start_weights(k, _, which):
        hbm, vmem = weights[which]
        part_of = pl.ds(k * nc, nc)
        pltpu.make_async_copy(hbm.at[part_of], vmem.at[part_of], w_sem.at[which]).start()
        return 0

    def weight_wait(which):
        hbm, vmem = weights[which]
        pltpu.make_async_copy(hbm, vmem, w_sem.at[which]).wait()

    barrier = pltpu.get_barrier_semaphore()
    peers = [t_peer(r) for r in range(1, tensors)] + [x_peer] + [z_peer(r) for r in range(1, zs)]
    with scope("start"):
        for peer in peers:
            pl.semaphore_signal(barrier, inc=1, device_id=peer, device_id_type=MESH)
        inputs = (
            pltpu.make_async_copy(s_hbm, s_raw, in_sem.at[0]),
            pltpu.make_async_copy(mw_hbm, mw_raw, in_sem.at[1]),
        )
        for copy in inputs:
            copy.start()
        for which in range(3):
            lax.fori_loop(0, chunks, functools.partial(start_weights, which=which), 0)
        for copy in inputs:
            copy.wait()
    with scope("relayout"):
        for j in range(streams):
            s_ref[j] = s_raw[:, j, :]
            mw_ref[j] = mw_raw[:, j, :]

    with scope("raw_logits"):
        raw = jnp.zeros((tok, mw_ref.shape[1]), jnp.float32)
        squares = jnp.zeros((tok, 1), jnp.float32)
        for j in range(streams):
            raw += contract_last(s_ref[j], mw_ref[j])
            wide = s_ref[j].astype(jnp.float32)
            squares += jnp.sum(wide * wide, axis=1, keepdims=True)
        count = raw.shape[1]
        part[...] = jnp.broadcast_to(squares, part.shape)
        part[:, :count] = raw
    with scope("barrier"):
        pl.semaphore_wait(barrier, len(peers))

    def a_copy(r):
        return send(part, part_in.at[r - 1], a_send.at[0], a_recv.at[0], t_peer(r))

    def a_all():
        return send(part_in, part_in, a_send.at[0], a_recv.at[0], t_peer(1))

    with scope("a_exchange"):
        for r in range(1, tensors):
            a_copy(r).start()
        a_all().wait_recv()
    with scope("gates"):
        total = part[...]
        for r in range(1, tensors):
            total = total + part_in[r - 1]
        scale_inv = lax.rsqrt(column(total, count) / width_all + epsilon)
        logits = total[:, :count] * scale_inv + bias_ref[...]
        gates = sigmoid(logits)
        mlp_input = column(gates, 0) * s_ref[0].astype(jnp.float32)
        for j in range(1, streams):
            mlp_input += column(gates, j) * s_ref[j].astype(jnp.float32)
        rows_all[slot_of(z)] = mlp_input.astype(jnp.bfloat16)

    mate, inner, outer = z_half * zb + 1 - z_odd, zb - z_half, (zs - 1) * (1 - z_half)

    def bz_copy(source, target):
        block = rows_all.at[slot_of(source)]
        return send(block, block, bz_send.at[0], bz_recv.at[source], z_dev(target))

    def bx_copy(source):
        at = slot_of(source)
        return send(rows_all.at[at], rows_all.at[zs + at], bx_send.at[0], bx_recv.at[0], x_peer)

    def bx_all():
        received = rows_all.at[pl.ds(zs, zs)]
        return send(received, received, bx_send.at[0], bx_recv.at[0], x_peer)

    with scope("b_start"):
        for target in (mate, outer, inner):
            bz_copy(z, target).start()
        bx_copy(z).start()
        for i in range(streams):
            post[i] = jnp.broadcast_to(2.0 * column(gates, streams + i), (tok, post.shape[2]))
    def turn(k, _, which):
        with scope("turn"):
            vmem = weights[which][1]
            span = pl.ds(pl.multiple_of(k * nc, nc), nc)
            for at in range(0, width, nc):
                vmem[span, at : at + nc] = vmem[span, at : at + nc].T
        return 0

    def turns(first, last):
        for which in range(2):
            low, high = (min(max(at - which * chunks, 0), chunks) for at in (first, last))
            if low < high:
                lax.fori_loop(low, high, functools.partial(turn, which=which), 0)

    weight_wait(0)
    turned = 0
    for at, source in enumerate((mate, inner, outer)):
        if at == 1:
            weight_wait(1)
        turns(turned, turned + TURNS[at])
        turned += TURNS[at]
        with scope(f"b_forward{at}"):
            bz_copy(source, source).wait_recv()
            bx_copy(source).start()
    turns(turned, 2 * chunks)

    with scope("sinkhorn"):
        entry[...] = jnp.zeros_like(entry)
        entry[:, :count] = jnp.exp(logits)
        flipped = entry[...].T
        first = 2 * streams
        mat = tuple(flipped[first + at : first + at + 1] for at in range(streams * streams))
        mat = lax.fori_loop(0, ITERS, functools.partial(sweep, streams), mat)
    with scope("mixed"):
        rest = jnp.zeros((LANES - len(mat), tok), jnp.float32)
        res = jnp.concatenate(mat + (rest,), axis=0).T
        for i in range(streams):
            line = column(res, i * streams) * s_ref[0].astype(jnp.float32)
            for j in range(1, streams):
                line += column(res, i * streams + j) * s_ref[j].astype(jnp.float32)
            mixed[i] = line
    with scope("b_wait"):
        bx_all().wait_recv()
        weight_wait(2)

    own_slot = core * ys + y

    def c1_copy(k):
        return send(sums.at[k, 1 - core], pair_in.at[k], c1_send.at[0], c1_recv.at[k], core_peer)

    def c2_copy(k, g, r):
        at = k * GROUPS + g
        return send(ring_out.at[at, r - 1], ring_in.at[at, r - 1], c2_send.at[0], c2_recv.at[at], y_peer(r))

    def c2_arrival(k, g):
        piece = ring_in.at[k * GROUPS + g]
        return send(piece, piece, c2_send.at[0], c2_recv.at[k * GROUPS + g], y_peer(1))

    def units(k):
        return pl.ds(pl.multiple_of(k * nc, nc), nc)

    def quarter(at):
        return pl.ds(pl.multiple_of(at * gq, gq), gq)

    def c3_copy(k, g, r, source):
        at = (k * GROUPS + g) * (ys - 1) + r - 1
        piece = hidden.at[g, core * ys + source, :, units(k)]
        return send(piece, piece, c3_send.at[0], c3_recv.at[at], y_peer(r))

    def c4_copy(k, g, source):
        piece = hidden.at[g, core * ys + source, :, units(k)]
        return send(piece, piece, c4_send.at[0], c4_recv.at[g], core_peer)

    def c4_arrival(g):
        piece = hidden.at[g, pl.ds((1 - core) * ys, ys)]
        return send(piece, piece, c4_send.at[0], c4_recv.at[g], core_peer)

    def c_first(k):
        with scope("c_first"):
            rows = rows_all[...].reshape(PAIR * zs * tok, width)
            shape = (PAIR, GROUPS, gh, nc)
            for at, vmem in ((pl.ds(0, nc), gate_v), (pl.ds(nc, nc), up_v)):
                product = None
                for kt in range(0, width, nc):
                    term = jnp.dot(rows[:, kt : kt + nc], vmem[pl.ds(k * nc, nc), kt : kt + nc], preferred_element_type=jnp.float32)
                    product = term if product is None else product + term
                sums[k, :, :, :, at] = product.reshape(shape)
            c1_copy(k).start()

    def c_second(g, k):
        with scope(f"c_second{g}"):
            if g == 0:
                c1_copy(k).wait_recv()
            for r in range(1, ys):
                at = quarter(y_at(r))
                both = sums[k, core, g, at] + pair_in[k, g, at]
                ring_out[k * GROUPS + g, r - 1] = both.astype(jnp.bfloat16)
                c2_copy(k, g, r).start()

    def c_third(g, k):
        with scope(f"c_third{g}"):
            at = quarter(y)
            both = sums[k, core, g, at] + pair_in[k, g, at]
            c2_arrival(k, g).wait_recv()
            for r in range(1, ys):
                both = both + ring_in[k * GROUPS + g, r - 1].astype(jnp.float32)
            gate, up = both[:, :nc], both[:, nc:]
            hidden[g, own_slot, :, units(k)] = (gate / (1.0 + jnp.exp(-gate)) * up).astype(jnp.bfloat16)
            for r in range(1, ys):
                c3_copy(k, g, r, y).start()
            c4_copy(k, g, y).start()

    def c_fourth(g, k):
        with scope(f"c_fourth{g}"):
            for r in range(1, ys):
                c3_copy(k, g, r, y_at(-r)).wait_recv()
                c4_copy(k, g, y_at(-r)).start()

    def pipeline(steps, stages):
        def step(t, _):
            for lag, count, stage in stages:
                @pl.when(jnp.logical_and(t >= lag, t < count + lag))
                def _():
                    stage(t - lag)

            return 0

        lax.fori_loop(0, steps, step, 0)

    late = min(LATE, chunks)
    second, third, fourth = (
        [functools.partial(stage, g) for g in range(GROUPS)] for stage in (c_second, c_third, c_fourth)
    )
    pipeline(
        chunks + LAG_FORWARD,
        (
            (0, chunks, c_first),
            (LAG_SUM[0], chunks, second[0]),
            (LAG_SUM[1], chunks, second[1]),
            (LAG_HIDDEN[0], chunks, third[0]),
            (LAG_HIDDEN[1], chunks, third[1]),
            (LAG_FORWARD, chunks, fourth[0]),
            (LAG_FORWARD + late, chunks - late, fourth[1]),
        ),
    )

    def cols(n):
        return pl.ds(pl.multiple_of(n * cc, cc), cc)

    def d1_copy(job):
        return send(cross_out.at[job], cross_in.at[job], d1_send.at[0], d1_recv.at[job], x_peer)

    def d2_copy(job, n, b, r):
        return send(line_out.at[job, b], line_in.at[n, r - 1], d2_send.at[0], d2_recv.at[n], z_peer(r))

    def d2_arrival(n):
        return send(line_in.at[n], line_in.at[n], d2_send.at[0], d2_recv.at[n], z_peer(1))

    def d_first(job):
        g, n = lax.div(job, columns), lax.rem(job, columns)

        @pl.when(n == 0)
        def _():
            with scope("c4_wait"):
                c4_arrival(g).wait_recv()

        def product(offset):
            rows = hidden[g].reshape(PAIR * gh, chunks * nc)
            return jnp.dot(rows, down_v[:, cols(n + offset)], preferred_element_type=jnp.float32)

        def finish(offset, value):
            own[job + offset] = value[:gh]
            cross_out[job + offset] = value[gh:].astype(jnp.bfloat16)
            d1_copy(job + offset).start()

        paired = columns // PAIR * PAIR

        @pl.when(jnp.logical_and(n < paired, lax.rem(n, PAIR) == 0))
        def _():
            with scope("d_first_pair"):
                values = [product(offset) for offset in range(PAIR)]
                for offset in range(PAIR):
                    finish(offset, values[offset])

        if paired < columns:
            @pl.when(n >= paired)
            def _():
                with scope("d_first"):
                    finish(0, product(0))

    def d_second(job):
        g, n = lax.div(job, columns), lax.rem(job, columns)
        with scope("d_second"):
            d1_copy(job).wait_recv()
            summed = (own[job] + cross_in[job].astype(jnp.float32)).reshape(zb, tok, cc)
            cross_sum[job] = summed
            line_out[job] = summed.astype(jnp.bfloat16)
            for b in range(zb):
                r = lax.rem(zb * b + lax.rem(b + g, GROUPS) - z + zs, zs)

                @pl.when(r > 0)
                def _():
                    d2_copy(job, n, b, r).start()

    def d_third(job):
        g, n = lax.div(job, columns), lax.rem(job, columns)

        @pl.when(g == own_group)
        def _():
            with scope("d_third"):
                mlp_out = cross_sum[job, z_half]
                d2_arrival(n).wait_recv()
                for r in range(1, zs):
                    mlp_out = mlp_out + line_in[n, r - 1].astype(jnp.float32)
                for i in range(streams):
                    value = mixed[i, :, cols(n)] + column(post[i], 0) * mlp_out
                    out_ref[i, :, cols(n)] = value.astype(jnp.bfloat16)

    jobs = GROUPS * columns
    pipeline(
        jobs + LAG_OUT,
        (
            (LAG_CROSS, jobs, d_second),
            (0, jobs, d_first),
            (1, late, lambda k: c_fourth(1, k + chunks - late)),
            (LAG_OUT, jobs, d_third),
        ),
    )

    with scope("drain"):
        a_all().wait_send()
        bx_all().wait_send()
        whole = [
            (rows_all.at[pl.ds(0, zs - 1)], bz_send),
            (pair_in, c1_send),
            (ring_in, c2_send),
            (hidden.at[:, pl.ds(0, ys - 1)], c3_send),
            (hidden.at[:, pl.ds(0, ys)], c4_send),
            (cross_in, d1_send),
            (line_in, d2_send),
        ]
        for ref, sem in whole:
            send(ref, ref, sem.at[0], sem.at[0], x_peer).wait_send()


def layer_scratch(zs, ys, tensors, tok, streams, logits, width, units, nc, cc):
    zb = zs // GROUPS
    gh = zb * tok
    gq = gh // ys
    chunks, columns = units // nc, width // cc
    jobs = GROUPS * columns
    f32, bf16 = jnp.float32, jnp.bfloat16
    arrays = [
        ((units, width), bf16),
        ((units, width), bf16),
        ((units, width), bf16),
        ((tok, streams, width), bf16),
        ((logits, streams, width), bf16),
        ((streams, tok, width), bf16),
        ((streams, logits, width), bf16),
        ((tok, LANES), f32),
        ((tensors - 1, tok, LANES), f32),
        ((tok, LANES), f32),
        ((streams, tok, LANES), f32),
        ((PAIR * zs, tok, width), bf16),
        ((streams, tok, width), f32),
        ((chunks, PAIR, GROUPS, gh, 2 * nc), f32),
        ((chunks, GROUPS, gh, 2 * nc), f32),
        ((chunks * GROUPS, ys - 1, gq, 2 * nc), bf16),
        ((chunks * GROUPS, ys - 1, gq, 2 * nc), bf16),
        ((GROUPS, PAIR * ys, gq, units), bf16),
        ((jobs, gh, cc), f32),
        ((jobs, gh, cc), bf16),
        ((jobs, gh, cc), bf16),
        ((jobs, zb, tok, cc), f32),
        ((jobs, zb, tok, cc), bf16),
        ((columns, zs - 1, tok, cc), bf16),
    ]
    sems = [(2,), (3,)]
    for count in (1, zs, 1, chunks, chunks * GROUPS, chunks * GROUPS * (ys - 1), GROUPS, jobs, columns):
        sems += [(1,), (count,)]
    size = sum(math.prod(shape) * jnp.dtype(kind).itemsize for shape, kind in arrays)
    return arrays, sems, size


def fused(mesh, streams, mix_weight, mix_bias, gate_weight, up_weight, down_weight):
    tok, stream_count, width = streams.shape
    units = gate_weight.shape[0]
    dps, tensors = mesh.shape["dp"], mesh.shape["tensor"]
    zs, ys = dps // PAIR, tensors // PAIR
    nc, cc = UNIT_CHUNK, COLUMN_CHUNK
    arrays, sems, _ = layer_scratch(zs, ys, tensors, tok, stream_count, mix_weight.shape[0], width, units, nc, cc)
    plan = (zs, ys, tensors, units // nc, nc, width // cc, cc, stream_count * width * tensors)
    bias = mix_bias[None, :]
    vmem = pl.BlockSpec(memory_space=pltpu.VMEM)
    hbm = pl.BlockSpec(memory_space=pl.ANY)
    out = pl.pallas_call(
        functools.partial(layer_kernel, plan),
        out_shape=pltpu.VMEM((stream_count, tok, width), jnp.bfloat16),
        in_specs=[hbm, hbm, vmem, hbm, hbm, hbm],
        out_specs=vmem,
        scratch_shapes=[pltpu.VMEM(shape, kind) for shape, kind in arrays]
        + [pltpu.SemaphoreType.DMA(shape) for shape in sems],
        compiler_params=pltpu.CompilerParams(
            collective_id=0, has_side_effects=True, vmem_limit_bytes=VMEM_BUDGET
        ),
    )(streams, mix_weight, bias, gate_weight, up_weight, down_weight)
    return out.transpose(1, 0, 2)


def fits(mesh, streams, mix_weight, gate_weight):
    tok, stream_count, width = streams.shape
    units = gate_weight.shape[0]
    dps, tensors = mesh.shape["dp"], mesh.shape["tensor"]
    if dps != PAIR * GROUPS * PAIR or tensors % PAIR or tensors < 2 * PAIR:
        return False
    zs, ys = dps // PAIR, tensors // PAIR
    if units % UNIT_CHUNK or width % COLUMN_CHUNK or tok % 16 or (zs // GROUPS * tok) % (16 * ys):
        return False
    if mix_weight.shape[0] >= LANES:
        return False
    size = layer_scratch(
        zs, ys, tensors, tok, stream_count, mix_weight.shape[0], width, units, UNIT_CHUNK, COLUMN_CHUNK
    )[2]
    return size < VMEM_BUDGET * 3 // 4


def solution(mesh):
    in_specs = (
        P("dp", None, "tensor"),
        P(None, None, "tensor"),
        P(),
        P("dp", "tensor"),
        P("dp", "tensor"),
        P("dp", "tensor"),
    )
    out_specs = P("dp", None, "tensor")

    def step(streams, mix_weight, mix_bias, gate_weight, up_weight, down_weight):
        operands = (streams, mix_weight, mix_bias, gate_weight, up_weight, down_weight)
        if fits(mesh, streams, mix_weight, gate_weight):
            return fused(mesh, *operands)
        return per_device(*operands)

    return jax.shard_map(step, mesh=mesh, in_specs=in_specs, out_specs=out_specs, check_vma=False)
```

```python
import functools
import math

import jax
import jax.numpy as jnp
from jax import lax
from jax.experimental import pallas as pl
from jax.experimental.pallas import tpu as pltpu
from jax.sharding import PartitionSpec as P

D = 7168
ITERS = 20


epsilon = 1e-06


def normalize(sweep_index, matrix):
    matrix = matrix / jnp.sum(matrix, axis=2, keepdims=True)
    return matrix / jnp.sum(matrix, axis=1, keepdims=True)


def mixing(raw_logits, squares, mix_bias, stream_count):
    scale_inv = lax.rsqrt(squares / (stream_count * D) + epsilon)
    logits = raw_logits * scale_inv[:, None] + mix_bias[None, :]
    pre_gate = jax.nn.sigmoid(logits[:, :stream_count])
    post_gate = 2.0 * jax.nn.sigmoid(logits[:, stream_count : 2 * stream_count])
    matrix = jnp.exp(logits[:, 2 * stream_count :]).reshape(-1, stream_count, stream_count)
    matrix = lax.fori_loop(0, ITERS, normalize, matrix)
    return (pre_gate, post_gate, matrix)


def contract_last(weights, rows):
    return lax.dot_general(
        weights, rows, (((1,), (1,)), ((), ())), preferred_element_type=jnp.float32
    )


def per_device(streams, mix_weight, mix_bias, gate_weight, up_weight, down_weight):
    tok_rows, stream_count, width_local = streams.shape
    logit_count = mix_weight.shape[0]
    flat_rows = streams.reshape(tok_rows, stream_count * width_local)
    flat_weight = mix_weight.reshape(logit_count, stream_count * width_local)
    raw_logits = lax.dot_general(
        flat_rows, flat_weight, (((1,), (1,)), ((), ())), preferred_element_type=jnp.float32
    )
    stream_wide = streams.astype(jnp.float32)
    squares = jnp.sum(stream_wide * stream_wide, axis=(1, 2))
    total_logits, total_squares = lax.psum((raw_logits, squares), "tensor")
    pre_gate, post_gate, res_mix = mixing(total_logits, total_squares, mix_bias, stream_count)
    mlp_input = jnp.einsum(
        "ts,tsc->tc", pre_gate, stream_wide, precision=lax.Precision.HIGHEST
    ).astype(jnp.bfloat16)
    unit_local = gate_weight.shape[0]
    block_rows = lax.all_gather(mlp_input, "dp", axis=0, tiled=True)
    gate_part = contract_last(gate_weight, block_rows)
    up_part = contract_last(up_weight, block_rows)
    both_parts = jnp.concatenate((gate_part, up_part), axis=0)
    unit_share = lax.psum_scatter(both_parts, "tensor", scatter_dimension=1, tiled=True)
    hidden_share = (jax.nn.silu(unit_share[:unit_local]) * unit_share[unit_local:]).astype(
        jnp.bfloat16
    )
    hidden = lax.all_gather(hidden_share, "tensor", axis=1, tiled=True)
    mlp_out = lax.psum_scatter(
        lax.dot_general(
            hidden, down_weight, (((0,), (0,)), ((), ())), preferred_element_type=jnp.float32
        ),
        "dp",
        scatter_dimension=0,
        tiled=True,
    )
    mixed = jnp.einsum("tij,tjc->tic", res_mix, stream_wide, precision=lax.Precision.HIGHEST)
    mixed = mixed + post_gate[:, :, None] * mlp_out[:, None, :]
    return mixed.astype(jnp.bfloat16)


MESH = pl.DeviceIdType.MESH
UNIT_CHUNK = 256
COLUMN_CHUNK = 256
PAIR = 2
GROUPS = 2
BODY = 3
LANES = 128
SUM_AT, HIDDEN_AT, FORWARD_AT = 1.99, 4.3, 6.5
FAR_GAP = 1.4
NEAR_DOWN = (10.75, 10.8, 11.0, 11.5)
VMEM_BUDGET = 58 * 1024 * 1024


def column(values, at):
    return values[:, at : at + 1]


def sigmoid(v):
    return 1.0 / (1.0 + jnp.exp(-v))


def sweep(count, _, entries):
    m = list(entries)
    for i in range(count):
        total_row = m[i * count]
        for j in range(1, count):
            total_row = total_row + m[i * count + j]
        inv = 1.0 / total_row
        for j in range(count):
            m[i * count + j] = m[i * count + j] * inv
    for j in range(count):
        total_col = m[j]
        for i in range(1, count):
            total_col = total_col + m[i * count + j]
        inv = 1.0 / total_col
        for i in range(count):
            m[i * count + j] = m[i * count + j] * inv
    return tuple(m)


def layer_kernel(
    plan,
    s_hbm,
    mw_hbm,
    bias_ref,
    gate_hbm,
    up_hbm,
    down_hbm,
    out_ref,
    gate_v,
    up_v,
    down_v,
    s_raw,
    mw_raw,
    s_ref,
    mw_ref,
    part,
    part_in,
    entry,
    logit_ref,
    post,
    rows_all,
    mixed,
    sums,
    pair_in,
    ring_out,
    ring_in,
    hidden,
    own,
    cross_out,
    cross_in,
    cross_sum,
    line_out,
    line_in,
    in_sem,
    w_sem,
    a_send,
    a_recv,
    bz_send,
    bz_recv,
    bx_send,
    bx_recv,
    c1_send,
    c1_recv,
    c2_send,
    c2_recv,
    c3_send,
    c3_recv,
    c4_send,
    c4_recv,
    d1_send,
    d1_recv,
    d2_send,
    d2_recv,
):
    zs, ys, tensors, chunks, nc, columns, cc, width_all = plan
    streams, tok, width = s_ref.shape
    scope = jax.named_scope
    dp = lax.axis_index("dp")
    tp = lax.axis_index("tensor")
    z, x = lax.div(dp, PAIR), lax.rem(dp, PAIR)
    y, core = lax.div(tp, PAIR), lax.rem(tp, PAIR)
    x_peer = (z * PAIR + 1 - x, tp)
    core_peer = (dp, y * PAIR + 1 - core)
    zb = zs // GROUPS
    gh = zb * tok
    gq = gh // ys
    z_half, z_odd = lax.div(z, zb), lax.rem(z, zb)

    def slot_of(source, target):
        apart = lax.rem(lax.div(source, zb) + lax.div(target, zb), GROUPS)
        return apart * PAIR * zb + lax.rem(source, zb)

    def y_at(r):
        return lax.rem(y + r + ys, ys)

    def z_dev(at):
        return (at * PAIR + x, tp)

    def z_peer(r):
        return z_dev(lax.rem(z + r + zs, zs))

    def block_peer(across, apart):
        at = z_half * zb + lax.rem(z_odd + apart, zb)
        return (at * PAIR + lax.rem(x + across, PAIR), tp)

    def y_peer(r):
        return (dp, y_at(r) * PAIR + core)

    def t_peer(r):
        return (dp, lax.rem(tp + r, tensors))

    def send(src, dst, ssem, rsem, peer):
        return pltpu.make_async_remote_copy(
            src_ref=src, dst_ref=dst, send_sem=ssem, recv_sem=rsem, device_id=peer, device_id_type=MESH
        )

    weights = ((gate_hbm, gate_v), (up_hbm, up_v), (down_hbm, down_v))

    def start_weights(k, _, which):
        hbm, vmem = weights[which]
        part_of = pl.ds(k * nc, nc)
        pltpu.make_async_copy(hbm.at[part_of], vmem.at[part_of], w_sem.at[which]).start()
        return 0

    def weight_wait(which):
        hbm, vmem = weights[which]
        pltpu.make_async_copy(hbm, vmem, w_sem.at[which]).wait()

    barrier = pltpu.get_barrier_semaphore()
    peers = [t_peer(r) for r in range(1, tensors)] + [x_peer, block_peer(1, 1)] + [z_peer(r) for r in range(1, zs)]
    with scope("start"):
        for peer in peers:
            pl.semaphore_signal(barrier, inc=1, device_id=peer, device_id_type=MESH)
        inputs = (
            pltpu.make_async_copy(s_hbm, s_raw, in_sem.at[0]),
            pltpu.make_async_copy(mw_hbm, mw_raw, in_sem.at[1]),
        )
        for copy in inputs:
            copy.start()
        for which in range(3):
            lax.fori_loop(0, chunks, functools.partial(start_weights, which=which), 0)
        for copy in inputs:
            copy.wait()
    with scope("relayout"):
        for j in range(streams):
            s_ref[j] = s_raw[:, j, :]
            mw_ref[j] = mw_raw[:, j, :]

    with scope("raw_logits"):
        raw = jnp.zeros((tok, mw_ref.shape[1]), jnp.float32)
        squares = jnp.zeros((tok, 1), jnp.float32)
        for j in range(streams):
            raw += contract_last(s_ref[j], mw_ref[j])
            wide = s_ref[j].astype(jnp.float32)
            squares += jnp.sum(wide * wide, axis=1, keepdims=True)
        count = raw.shape[1]
        part[...] = jnp.broadcast_to(squares, part.shape)
        part[:, :count] = raw
    with scope("barrier"):
        pl.semaphore_wait(barrier, len(peers))

    def a_copy(r):
        return send(part, part_in.at[r - 1], a_send.at[0], a_recv.at[0], t_peer(r))

    def a_all():
        return send(part_in, part_in, a_send.at[0], a_recv.at[0], t_peer(1))

    with scope("a_exchange"):
        for r in range(1, tensors):
            a_copy(r).start()
        a_all().wait_recv()
    with scope("gates"):
        total = part[...]
        for r in range(1, tensors):
            total = total + part_in[r - 1]
        scale_inv = lax.rsqrt(column(total, count) / width_all + epsilon)
        logits = total[:, :count] * scale_inv + bias_ref[...]
        logit_ref[:, :count] = logits
        gates = sigmoid(logits)
        mlp_input = column(gates, 0) * s_ref[0].astype(jnp.float32)
        for j in range(1, streams):
            mlp_input += column(gates, j) * s_ref[j].astype(jnp.float32)
        rows_all[slot_of(z, z)] = mlp_input.astype(jnp.bfloat16)

    mate, inner, outer = z_half * zb + 1 - z_odd, zb - z_half, (zs - 1) * (1 - z_half)

    def bz_copy(source, target):
        src, dst = rows_all.at[slot_of(source, source)], rows_all.at[slot_of(source, target)]
        return send(src, dst, bz_send.at[0], bz_recv.at[source], z_dev(target))

    def bz_arrival(source):
        block = rows_all.at[slot_of(source, z)]
        return send(block, block, bz_send.at[0], bz_recv.at[source], z_dev(source))

    def bx_copy(source, g):
        at = slot_of(source, z)
        return send(rows_all.at[at], rows_all.at[at + zb], bx_send.at[0], bx_recv.at[g], x_peer)

    def bx_all(g):
        received = rows_all.at[pl.ds((g * PAIR + 1) * zb, zb)]
        return send(received, received, bx_send.at[0], bx_recv.at[g], x_peer)

    def bx_mate():
        src, dst = rows_all.at[slot_of(z, z)], rows_all.at[slot_of(z, mate) + zb]
        return send(src, dst, bx_send.at[0], bx_recv.at[0], block_peer(1, 1))

    with scope("b_start"):
        bz_copy(z, mate).start()
        bx_mate().start()
        bx_copy(z, 0).start()
        for target in (outer, inner):
            bz_copy(z, target).start()
        for i in range(streams):
            post[i] = jnp.broadcast_to(2.0 * column(gates, streams + i), (tok, post.shape[2]))

    def turn(k, _, which):
        with scope("turn"):
            vmem = weights[which][1]
            span = pl.ds(pl.multiple_of(k * nc, nc), nc)
            for at in range(0, width, nc):
                vmem[span, at : at + nc] = vmem[span, at : at + nc].T
        return 0

    for which in range(2):
        weight_wait(which)
        lax.fori_loop(0, chunks, functools.partial(turn, which=which), 0)
    with scope("b_wait"):
        bz_arrival(mate).wait_recv()
        bx_all(0).wait_recv()

    def forward(_):
        with scope("b_forward"):
            for source in (inner, outer):
                bz_arrival(source).wait_recv()
                bx_copy(source, 1).start()

    def streams_mixed(_):
        with scope("sinkhorn"):
            entry[...] = jnp.zeros_like(entry)
            entry[:, :count] = jnp.exp(logit_ref[:, :count])
            flipped = entry[...].T
            first = 2 * streams
            mat = tuple(flipped[first + at : first + at + 1] for at in range(streams * streams))
            mat = lax.fori_loop(0, ITERS, functools.partial(sweep, streams), mat)
        with scope("mixed"):
            rest = jnp.zeros((LANES - len(mat), tok), jnp.float32)
            res = jnp.concatenate(mat + (rest,), axis=0).T
            for i in range(streams):
                line = column(res, i * streams) * s_ref[0].astype(jnp.float32)
                for j in range(1, streams):
                    line += column(res, i * streams + j) * s_ref[j].astype(jnp.float32)
                mixed[i] = line

    own_slot = core * ys + y

    def units(job):
        return pl.ds(pl.multiple_of(lax.rem(job, chunks) * nc, nc), nc)

    def quarter(at):
        return pl.ds(pl.multiple_of(at * gq, gq), gq)

    def c1_copy(job):
        span = pl.ds(job, BODY)
        return send(sums.at[span, 1 - core], pair_in.at[span], c1_send.at[0], c1_recv.at[lax.div(job, BODY)], core_peer)

    def c2_copy(job, r):
        return send(ring_out.at[job, r - 1], ring_in.at[job, r - 1], c2_send.at[0], c2_recv.at[job], y_peer(r))

    def c2_arrival(job):
        return send(ring_in.at[job], ring_in.at[job], c2_send.at[0], c2_recv.at[job], y_peer(1))

    def c3_copy(job, r, source):
        piece = hidden.at[lax.div(job, chunks), core * ys + source, :, units(job)]
        return send(piece, piece, c3_send.at[0], c3_recv.at[job * (ys - 1) + r - 1], y_peer(r))

    def c4_copy(job, source):
        g = lax.div(job, chunks)
        piece = hidden.at[g, core * ys + source, :, units(job)]
        return send(piece, piece, c4_send.at[0], c4_recv.at[g], core_peer)

    def c4_arrival(g):
        piece = hidden.at[g, pl.ds((1 - core) * ys, ys)]
        return send(piece, piece, c4_send.at[0], c4_recv.at[g], core_peer)

    def far_wait(_):
        with scope("far_wait"):
            bx_all(1).wait_recv()

    def c_first(job):
        with scope("c_first"):
            g = job // chunks
            rows = rows_all[pl.ds(g * PAIR * zb, PAIR * zb)].reshape(PAIR * gh, width)
            for i in range(BODY):
                for at, vmem in ((pl.ds(0, nc), gate_v), (pl.ds(nc, nc), up_v)):
                    product = None
                    for kt in range(0, width, nc):
                        block = vmem[units(job + i), kt : kt + nc]
                        term = jnp.dot(rows[:, kt : kt + nc], block, preferred_element_type=jnp.float32)
                        product = term if product is None else product + term
                    sums[job + i, :, :, at] = product.reshape(PAIR, gh, nc)
            c1_copy(job).start()

    def c_second(job):
        with scope("c_second"):
            for r in range(1, ys):
                at = quarter(y_at(r))
                both = sums[job, core, at] + pair_in[job, at]
                ring_out[job, r - 1] = both.astype(jnp.bfloat16)
                c2_copy(job, r).start()

    def c_third(job):
        with scope("c_third"):
            at = quarter(y)
            both = sums[job, core, at] + pair_in[job, at]
            c2_arrival(job).wait_recv()
            for r in range(1, ys):
                both = both + ring_in[job, r - 1].astype(jnp.float32)
            gate, up = both[:, :nc], both[:, nc:]
            g = lax.div(job, chunks)
            hidden[g, own_slot, :, units(job)] = (gate / (1.0 + jnp.exp(-gate)) * up).astype(jnp.bfloat16)
            for r in range(1, ys):
                c3_copy(job, r, y).start()
            c4_copy(job, y).start()

    def c_fourth(job):
        with scope("c_fourth"):
            for r in range(1, ys):
                c3_copy(job, r, y_at(-r)).wait_recv()
                c4_copy(job, y_at(-r)).start()

    def run(stage, first, count):
        def body(job, _):
            stage(job)
            return 0

        lax.fori_loop(first, first + count, body, 0)

    def cols(n):
        return pl.ds(pl.multiple_of(n * cc, cc), cc)

    def d1_copy(job, r):
        across, apart = r // zb, r % zb
        piece = cross_out.at[job, across * zb + lax.rem(z_odd + apart, zb)]
        return send(piece, cross_in.at[job, r - 1], d1_send.at[0], d1_recv.at[job], block_peer(across, apart))

    def d1_arrival(job):
        return send(cross_in.at[job], cross_in.at[job], d1_send.at[0], d1_recv.at[job], x_peer)

    def d2_copy(n):
        return send(line_out.at[n], line_in.at[n], d2_send.at[0], d2_recv.at[n], z_peer(zb))

    def d_first(g, n, width_of):
        with scope("d_first"):
            rows = hidden[g].reshape(PAIR * gh, chunks * nc)
            values = [
                jnp.dot(rows, down_v[:, (n + i) * cc : (n + i + 1) * cc], preferred_element_type=jnp.float32)
                for i in range(width_of)
            ]
            for i, value in enumerate(values):
                job = g * columns + n + i
                value = value.reshape(PAIR * zb, tok, cc)
                own[job] = value
                cross_out[job] = value.astype(jnp.bfloat16)
                for r in range(1, PAIR * zb):
                    d1_copy(job, r).start()

    alone = columns % PAIR
    parts = [(0, alone)] * (alone > 0) + [(n, PAIR) for n in range(alone, columns, PAIR)]

    def block_sum(job):
        total = own[job, z_odd]
        d1_arrival(job).wait_recv()
        for r in range(1, PAIR * zb):
            total = total + cross_in[job, r - 1].astype(jnp.float32)
        return total

    def d_near(n):
        with scope("d_near"):
            cross_sum[n] = block_sum(n)

    def d_far(n):
        with scope("d_far"):
            line_out[n] = block_sum(n + columns).astype(jnp.bfloat16)
            d2_copy(n).start()

    def d_third(n):
        with scope("d_third"):
            mlp_out = cross_sum[n]
            d2_copy(n).wait_recv()
            mlp_out = mlp_out + line_in[n].astype(jnp.float32)
            for i in range(streams):
                value = mixed[i, :, cols(n)] + column(post[i], 0) * mlp_out
                out_ref[i, :, cols(n)] = value.astype(jnp.bfloat16)

    def sum_triple(job):
        with scope("c1_wait"):
            c1_copy(job).wait_recv()
        run(c_second, job, BODY)

    def near_ready(_):
        with scope("c4_wait"):
            c4_arrival(0).wait_recv()
            weight_wait(2)

    triples = chunks // BODY
    base = triples + FAR_GAP
    timed = [(0.5, forward, 0), (triples + 0.2, streams_mixed, 0), (base - 0.01, far_wait, 0)]
    for g, origin in enumerate((0, base)):
        for i in range(triples):
            job = g * chunks + i * BODY
            timed += [
                (origin + i, c_first, job),
                (origin + i + SUM_AT, sum_triple, job),
                (origin + i + HIDDEN_AT, functools.partial(run, c_third, count=BODY), job),
                (origin + i + FORWARD_AT, functools.partial(run, c_fourth, count=BODY), job),
            ]
    for i, (n, count_of) in enumerate(parts):
        at = NEAR_DOWN[min(i, len(NEAR_DOWN) - 1)]
        if i == 0:
            timed.append((at - 0.01, near_ready, 0))
        timed.append((at, lambda _, n=n, count_of=count_of: d_first(0, n, count_of), 0))
    for _, stage, job in sorted(timed, key=lambda item: item[0]):
        if isinstance(stage, functools.partial):
            stage(first=job)
        else:
            stage(job)

    with scope("c4_wait"):
        c4_arrival(1).wait_recv()
    for n, count_of in parts:
        d_first(1, n, count_of)
    run(d_near, 0, columns)
    run(d_far, 0, columns)
    run(d_third, 0, columns)

    with scope("drain"):
        a_all().wait_send()
        for g in range(GROUPS):
            bx_all(g).wait_send()
        whole = [
            (rows_all.at[pl.ds(0, zs - 1)], bz_send),
            (pair_in, c1_send),
            (ring_in, c2_send),
            (hidden.at[:, pl.ds(0, ys - 1)], c3_send),
            (hidden.at[:, pl.ds(0, ys)], c4_send),
            (cross_in, d1_send),
            (line_in, d2_send),
        ]
        for ref, sem in whole:
            send(ref, ref, sem.at[0], sem.at[0], x_peer).wait_send()


def layer_scratch(zs, ys, tensors, tok, streams, logits, width, units, nc, cc):
    zb = zs // GROUPS
    gh = zb * tok
    gq = gh // ys
    chunks, columns = units // nc, width // cc
    jobs = GROUPS * columns
    f32, bf16 = jnp.float32, jnp.bfloat16
    arrays = [
        ((units, width), bf16),
        ((units, width), bf16),
        ((units, width), bf16),
        ((tok, streams, width), bf16),
        ((logits, streams, width), bf16),
        ((streams, tok, width), bf16),
        ((streams, logits, width), bf16),
        ((tok, LANES), f32),
        ((tensors - 1, tok, LANES), f32),
        ((tok, LANES), f32),
        ((tok, LANES), f32),
        ((streams, tok, LANES), f32),
        ((PAIR * zs, tok, width), bf16),
        ((streams, tok, width), f32),
        ((chunks * GROUPS, PAIR, gh, 2 * nc), f32),
        ((chunks * GROUPS, gh, 2 * nc), f32),
        ((chunks * GROUPS, ys - 1, gq, 2 * nc), bf16),
        ((chunks * GROUPS, ys - 1, gq, 2 * nc), bf16),
        ((GROUPS, PAIR * ys, gq, units), bf16),
        ((jobs, PAIR * zb, tok, cc), f32),
        ((jobs, PAIR * zb, tok, cc), bf16),
        ((jobs, PAIR * zb - 1, tok, cc), bf16),
        ((columns, tok, cc), f32),
        ((columns, tok, cc), bf16),
        ((columns, tok, cc), bf16),
    ]
    sems = [(2,), (3,)]
    for count in (1, zs, GROUPS, chunks * GROUPS // BODY, chunks * GROUPS, chunks * GROUPS * (ys - 1), GROUPS, jobs, columns):
        sems += [(1,), (count,)]
    size = sum(math.prod(shape) * jnp.dtype(kind).itemsize for shape, kind in arrays)
    return arrays, sems, size


def fused(mesh, streams, mix_weight, mix_bias, gate_weight, up_weight, down_weight):
    tok, stream_count, width = streams.shape
    units = gate_weight.shape[0]
    dps, tensors = mesh.shape["dp"], mesh.shape["tensor"]
    zs, ys = dps // PAIR, tensors // PAIR
    nc, cc = UNIT_CHUNK, COLUMN_CHUNK
    arrays, sems, _ = layer_scratch(zs, ys, tensors, tok, stream_count, mix_weight.shape[0], width, units, nc, cc)
    plan = (zs, ys, tensors, units // nc, nc, width // cc, cc, stream_count * width * tensors)
    bias = mix_bias[None, :]
    vmem = pl.BlockSpec(memory_space=pltpu.VMEM)
    hbm = pl.BlockSpec(memory_space=pl.ANY)
    out = pl.pallas_call(
        functools.partial(layer_kernel, plan),
        out_shape=pltpu.VMEM((stream_count, tok, width), jnp.bfloat16),
        in_specs=[hbm, hbm, vmem, hbm, hbm, hbm],
        out_specs=vmem,
        scratch_shapes=[pltpu.VMEM(shape, kind) for shape, kind in arrays]
        + [pltpu.SemaphoreType.DMA(shape) for shape in sems],
        compiler_params=pltpu.CompilerParams(
            collective_id=0, has_side_effects=True, vmem_limit_bytes=VMEM_BUDGET
        ),
    )(streams, mix_weight, bias, gate_weight, up_weight, down_weight)
    return out.transpose(1, 0, 2)


def fits(mesh, streams, mix_weight, gate_weight):
    tok, stream_count, width = streams.shape
    units = gate_weight.shape[0]
    dps, tensors = mesh.shape["dp"], mesh.shape["tensor"]
    if dps != PAIR * GROUPS * PAIR or tensors % PAIR or tensors < 2 * PAIR:
        return False
    zs, ys = dps // PAIR, tensors // PAIR
    if units % (BODY * UNIT_CHUNK) or width % UNIT_CHUNK or width % COLUMN_CHUNK or tok % 16 or (zs // GROUPS * tok) % (16 * ys):
        return False
    if mix_weight.shape[0] >= LANES:
        return False
    size = layer_scratch(
        zs, ys, tensors, tok, stream_count, mix_weight.shape[0], width, units, UNIT_CHUNK, COLUMN_CHUNK
    )[2]
    return size < VMEM_BUDGET * 3 // 4


def solution(mesh):
    in_specs = (
        P("dp", None, "tensor"),
        P(None, None, "tensor"),
        P(),
        P("dp", "tensor"),
        P("dp", "tensor"),
        P("dp", "tensor"),
    )
    out_specs = P("dp", None, "tensor")

    def step(streams, mix_weight, mix_bias, gate_weight, up_weight, down_weight):
        operands = (streams, mix_weight, mix_bias, gate_weight, up_weight, down_weight)
        if fits(mesh, streams, mix_weight, gate_weight):
            return fused(mesh, *operands)
        return per_device(*operands)

    return jax.shard_map(step, mesh=mesh, in_specs=in_specs, out_specs=out_specs, check_vma=False)
```

```python
import functools
import math

import jax
import jax.numpy as jnp
from jax import lax
from jax.experimental import pallas as pl
from jax.experimental.pallas import tpu as pltpu
from jax.sharding import PartitionSpec as P

D = 7168
ITERS = 20


epsilon = 1e-06


def normalize(sweep_index, matrix):
    matrix = matrix / jnp.sum(matrix, axis=2, keepdims=True)
    return matrix / jnp.sum(matrix, axis=1, keepdims=True)


def mixing(raw_logits, squares, mix_bias, stream_count):
    scale_inv = lax.rsqrt(squares / (stream_count * D) + epsilon)
    logits = raw_logits * scale_inv[:, None] + mix_bias[None, :]
    pre_gate = jax.nn.sigmoid(logits[:, :stream_count])
    post_gate = 2.0 * jax.nn.sigmoid(logits[:, stream_count : 2 * stream_count])
    matrix = jnp.exp(logits[:, 2 * stream_count :]).reshape(-1, stream_count, stream_count)
    matrix = lax.fori_loop(0, ITERS, normalize, matrix)
    return (pre_gate, post_gate, matrix)


def contract_last(weights, rows):
    return lax.dot_general(
        weights, rows, (((1,), (1,)), ((), ())), preferred_element_type=jnp.float32
    )


def per_device(streams, mix_weight, mix_bias, gate_weight, up_weight, down_weight):
    tok_rows, stream_count, width_local = streams.shape
    logit_count = mix_weight.shape[0]
    flat_rows = streams.reshape(tok_rows, stream_count * width_local)
    flat_weight = mix_weight.reshape(logit_count, stream_count * width_local)
    raw_logits = lax.dot_general(
        flat_rows, flat_weight, (((1,), (1,)), ((), ())), preferred_element_type=jnp.float32
    )
    stream_wide = streams.astype(jnp.float32)
    squares = jnp.sum(stream_wide * stream_wide, axis=(1, 2))
    total_logits, total_squares = lax.psum((raw_logits, squares), "tensor")
    pre_gate, post_gate, res_mix = mixing(total_logits, total_squares, mix_bias, stream_count)
    mlp_input = jnp.einsum(
        "ts,tsc->tc", pre_gate, stream_wide, precision=lax.Precision.HIGHEST
    ).astype(jnp.bfloat16)
    unit_local = gate_weight.shape[0]
    block_rows = lax.all_gather(mlp_input, "dp", axis=0, tiled=True)
    gate_part = contract_last(gate_weight, block_rows)
    up_part = contract_last(up_weight, block_rows)
    both_parts = jnp.concatenate((gate_part, up_part), axis=0)
    unit_share = lax.psum_scatter(both_parts, "tensor", scatter_dimension=1, tiled=True)
    hidden_share = (jax.nn.silu(unit_share[:unit_local]) * unit_share[unit_local:]).astype(
        jnp.bfloat16
    )
    hidden = lax.all_gather(hidden_share, "tensor", axis=1, tiled=True)
    mlp_out = lax.psum_scatter(
        lax.dot_general(
            hidden, down_weight, (((0,), (0,)), ((), ())), preferred_element_type=jnp.float32
        ),
        "dp",
        scatter_dimension=0,
        tiled=True,
    )
    mixed = jnp.einsum("tij,tjc->tic", res_mix, stream_wide, precision=lax.Precision.HIGHEST)
    mixed = mixed + post_gate[:, :, None] * mlp_out[:, None, :]
    return mixed.astype(jnp.bfloat16)


MESH = pl.DeviceIdType.MESH
UNIT_CHUNK = 256
COLUMN_CHUNK = 256
PAIR = 2
GROUPS = 2
BODY = 3
LANES = 128
SUM_AT, HIDDEN_AT, FORWARD_AT = (0.99, 0.99), 3.3, 5.5
NEAR_HIDDEN, NEAR_FORWARD = 4.1, 6.33
FAR_GAP = 0.5
VMEM_BUDGET = 58 * 1024 * 1024


def column(values, at):
    return values[:, at : at + 1]


def sigmoid(v):
    return 1.0 / (1.0 + jnp.exp(-v))


def sweep(count, _, entries):
    m = list(entries)
    for i in range(count):
        total_row = m[i * count]
        for j in range(1, count):
            total_row = total_row + m[i * count + j]
        inv = 1.0 / total_row
        for j in range(count):
            m[i * count + j] = m[i * count + j] * inv
    for j in range(count):
        total_col = m[j]
        for i in range(1, count):
            total_col = total_col + m[i * count + j]
        inv = 1.0 / total_col
        for i in range(count):
            m[i * count + j] = m[i * count + j] * inv
    return tuple(m)


def layer_kernel(
    plan,
    s_hbm,
    mw_hbm,
    bias_ref,
    gate_hbm,
    up_hbm,
    down_hbm,
    out_ref,
    gate_v,
    up_v,
    down_v,
    s_raw,
    mw_raw,
    s_ref,
    mw_ref,
    part,
    part_in,
    entry,
    logit_ref,
    post,
    rows_all,
    mixed,
    sums,
    pair_in,
    ring_out,
    ring_in,
    hidden,
    own,
    cross_out,
    cross_in,
    cross_sum,
    line_out,
    line_in,
    in_sem,
    w_sem,
    a_send,
    a_recv,
    bz_send,
    bz_recv,
    bx_send,
    bx_recv,
    c1_send,
    c1_recv,
    c2_send,
    c2_recv,
    c3_send,
    c3_recv,
    c4_send,
    c4_recv,
    d1_send,
    d1_recv,
    d2_send,
    d2_recv,
):
    zs, ys, tensors, chunks, nc, columns, cc, width_all = plan
    streams, tok, width = s_ref.shape
    scope = jax.named_scope
    dp = lax.axis_index("dp")
    tp = lax.axis_index("tensor")
    z, x = lax.div(dp, PAIR), lax.rem(dp, PAIR)
    y, core = lax.div(tp, PAIR), lax.rem(tp, PAIR)
    x_peer = (z * PAIR + 1 - x, tp)
    core_peer = (dp, y * PAIR + 1 - core)
    zb = zs // GROUPS
    gh = zb * tok
    gq = gh // ys
    z_half, z_odd = lax.div(z, zb), lax.rem(z, zb)

    def slot_of(source, target):
        apart = lax.rem(lax.div(source, zb) + lax.div(target, zb), GROUPS)
        return apart * PAIR * zb + lax.rem(source, zb)

    def y_at(r):
        return lax.rem(y + r + ys, ys)

    def z_dev(at):
        return (at * PAIR + x, tp)

    def z_peer(r):
        return z_dev(lax.rem(z + r + zs, zs))

    def block_peer(across, apart):
        at = z_half * zb + lax.rem(z_odd + apart, zb)
        return (at * PAIR + lax.rem(x + across, PAIR), tp)

    def y_peer(r):
        return (dp, y_at(r) * PAIR + core)

    def t_peer(r):
        return (dp, lax.rem(tp + r, tensors))

    def send(src, dst, ssem, rsem, peer):
        return pltpu.make_async_remote_copy(
            src_ref=src, dst_ref=dst, send_sem=ssem, recv_sem=rsem, device_id=peer, device_id_type=MESH
        )

    weights = ((gate_hbm, gate_v), (up_hbm, up_v), (down_hbm, down_v))

    def start_weights(k, _, which):
        hbm, vmem = weights[which]
        part_of = pl.ds(k * nc, nc)
        pltpu.make_async_copy(hbm.at[part_of], vmem.at[part_of], w_sem.at[which]).start()
        return 0

    def weight_wait(which):
        hbm, vmem = weights[which]
        pltpu.make_async_copy(hbm, vmem, w_sem.at[which]).wait()

    barrier = pltpu.get_barrier_semaphore()
    peers = [t_peer(r) for r in range(1, tensors)] + [x_peer, block_peer(1, 1)] + [z_peer(r) for r in range(1, zs)]
    with scope("start"):
        for peer in peers:
            pl.semaphore_signal(barrier, inc=1, device_id=peer, device_id_type=MESH)
        inputs = (
            pltpu.make_async_copy(s_hbm, s_raw, in_sem.at[0]),
            pltpu.make_async_copy(mw_hbm, mw_raw, in_sem.at[1]),
        )
        for copy in inputs:
            copy.start()
        for which in range(3):
            lax.fori_loop(0, chunks, functools.partial(start_weights, which=which), 0)
        for copy in inputs:
            copy.wait()
    with scope("relayout"):
        for j in range(streams):
            s_ref[j] = s_raw[:, j, :]
            mw_ref[j] = mw_raw[:, j, :]

    with scope("raw_logits"):
        raw = jnp.zeros((tok, mw_ref.shape[1]), jnp.float32)
        squares = jnp.zeros((tok, 1), jnp.float32)
        for j in range(streams):
            raw += contract_last(s_ref[j], mw_ref[j])
            wide = s_ref[j].astype(jnp.float32)
            squares += jnp.sum(wide * wide, axis=1, keepdims=True)
        count = raw.shape[1]
        part[...] = jnp.broadcast_to(squares, part.shape)
        part[:, :count] = raw
    with scope("barrier"):
        pl.semaphore_wait(barrier, len(peers))

    def a_copy(r):
        return send(part, part_in.at[r - 1], a_send.at[0], a_recv.at[0], t_peer(r))

    def a_all():
        return send(part_in, part_in, a_send.at[0], a_recv.at[0], t_peer(1))

    with scope("a_exchange"):
        for r in range(1, tensors):
            a_copy(r).start()
        a_all().wait_recv()
    with scope("gates"):
        total = part[...]
        for r in range(1, tensors):
            total = total + part_in[r - 1]
        scale_inv = lax.rsqrt(column(total, count) / width_all + epsilon)
        logits = total[:, :count] * scale_inv + bias_ref[...]
        logit_ref[:, :count] = logits
        gates = sigmoid(logits)
        mlp_input = column(gates, 0) * s_ref[0].astype(jnp.float32)
        for j in range(1, streams):
            mlp_input += column(gates, j) * s_ref[j].astype(jnp.float32)
        rows_all[slot_of(z, z)] = mlp_input.astype(jnp.bfloat16)

    mate, inner, outer = z_half * zb + 1 - z_odd, zb - z_half, (zs - 1) * (1 - z_half)

    def bz_copy(source, target):
        src, dst = rows_all.at[slot_of(source, source)], rows_all.at[slot_of(source, target)]
        return send(src, dst, bz_send.at[0], bz_recv.at[source], z_dev(target))

    def bz_arrival(source):
        block = rows_all.at[slot_of(source, z)]
        return send(block, block, bz_send.at[0], bz_recv.at[source], z_dev(source))

    def bx_copy(source, g):
        at = slot_of(source, z)
        return send(rows_all.at[at], rows_all.at[at + zb], bx_send.at[0], bx_recv.at[g], x_peer)

    def bx_all(g):
        received = rows_all.at[pl.ds((g * PAIR + 1) * zb, zb)]
        return send(received, received, bx_send.at[0], bx_recv.at[g], x_peer)

    def bx_mate():
        src, dst = rows_all.at[slot_of(z, z)], rows_all.at[slot_of(z, mate) + zb]
        return send(src, dst, bx_send.at[0], bx_recv.at[0], block_peer(1, 1))

    with scope("b_start"):
        bz_copy(z, mate).start()
        bx_copy(z, 0).start()
        for target in (outer, inner):
            bz_copy(z, target).start()
        bx_mate().start()
        for i in range(streams):
            post[i] = jnp.broadcast_to(2.0 * column(gates, streams + i), (tok, post.shape[2]))

    def turn(k, _, which):
        with scope("turn"):
            vmem = weights[which][1]
            span = pl.ds(pl.multiple_of(k * nc, nc), nc)
            for at in range(0, width, nc):
                vmem[span, at : at + nc] = vmem[span, at : at + nc].T
        return 0

    for which in range(2):
        weight_wait(which)
        lax.fori_loop(0, chunks, functools.partial(turn, which=which), 0)
    def forward(source):
        with scope("b_forward"):
            bz_arrival(source).wait_recv()
            bx_copy(source, 1).start()

    def streams_mixed(_):
        with scope("sinkhorn"):
            entry[...] = jnp.zeros_like(entry)
            entry[:, :count] = jnp.exp(logit_ref[:, :count])
            flipped = entry[...].T
            first = 2 * streams
            mat = tuple(flipped[first + at : first + at + 1] for at in range(streams * streams))
            mat = lax.fori_loop(0, ITERS, functools.partial(sweep, streams), mat)
        with scope("mixed"):
            rest = jnp.zeros((LANES - len(mat), tok), jnp.float32)
            res = jnp.concatenate(mat + (rest,), axis=0).T
            for i in range(streams):
                line = column(res, i * streams) * s_ref[0].astype(jnp.float32)
                for j in range(1, streams):
                    line += column(res, i * streams + j) * s_ref[j].astype(jnp.float32)
                mixed[i] = line

    own_slot = core * ys + y

    def units(job):
        return pl.ds(pl.multiple_of(lax.rem(job, chunks) * nc, nc), nc)

    def quarter(at):
        return pl.ds(pl.multiple_of(at * gq, gq), gq)

    def c1_copy(job, size):
        span = pl.ds(job, size)
        return send(sums.at[span, 1 - core], pair_in.at[span], c1_send.at[0], c1_recv.at[job], core_peer)

    def c2_copy(job, r):
        return send(ring_out.at[job, r - 1], ring_in.at[job, r - 1], c2_send.at[0], c2_recv.at[job], y_peer(r))

    def c2_arrival(job):
        return send(ring_in.at[job], ring_in.at[job], c2_send.at[0], c2_recv.at[job], y_peer(1))

    def c3_copy(job, r, source):
        piece = hidden.at[lax.div(job, chunks), core * ys + source, :, units(job)]
        return send(piece, piece, c3_send.at[0], c3_recv.at[job * (ys - 1) + r - 1], y_peer(r))

    def c4_copy(job, source):
        g = lax.div(job, chunks)
        piece = hidden.at[g, core * ys + source, :, units(job)]
        return send(piece, piece, c4_send.at[0], c4_recv.at[g], core_peer)

    def c4_arrival(g):
        piece = hidden.at[g, pl.ds((1 - core) * ys, ys)]
        return send(piece, piece, c4_send.at[0], c4_recv.at[g], core_peer)

    def far_wait(_):
        with scope("far_wait"):
            bx_all(1).wait_recv()

    def c_first(job, size):
        with scope("c_first"):
            g = job // chunks
            rows = rows_all[pl.ds(g * PAIR * zb, PAIR * zb)].reshape(PAIR * gh, width)
            for i in range(size):
                for at, vmem in ((pl.ds(0, nc), gate_v), (pl.ds(nc, nc), up_v)):
                    product = None
                    for kt in range(0, width, nc):
                        block = vmem[units(job + i), kt : kt + nc]
                        term = jnp.dot(rows[:, kt : kt + nc], block, preferred_element_type=jnp.float32)
                        product = term if product is None else product + term
                    sums[job + i, :, :, at] = product.reshape(PAIR, gh, nc)
            c1_copy(job, size).start()

    def c_second(job):
        with scope("c_second"):
            for r in range(1, ys):
                at = quarter(y_at(r))
                both = sums[job, core, at] + pair_in[job, at]
                ring_out[job, r - 1] = both.astype(jnp.bfloat16)
                c2_copy(job, r).start()

    def c_third(job):
        with scope("c_third"):
            at = quarter(y)
            both = sums[job, core, at] + pair_in[job, at]
            c2_arrival(job).wait_recv()
            for r in range(1, ys):
                both = both + ring_in[job, r - 1].astype(jnp.float32)
            gate, up = both[:, :nc], both[:, nc:]
            g = lax.div(job, chunks)
            hidden[g, own_slot, :, units(job)] = (gate / (1.0 + jnp.exp(-gate)) * up).astype(jnp.bfloat16)
            for r in range(1, ys):
                c3_copy(job, r, y).start()
            c4_copy(job, y).start()

    def c_fourth(job):
        with scope("c_fourth"):
            for r in range(1, ys):
                c3_copy(job, r, y_at(-r)).wait_recv()
                c4_copy(job, y_at(-r)).start()

    def run(stage, first, count):
        def body(job, _):
            stage(job)
            return 0

        lax.fori_loop(first, first + count, body, 0)

    def cols(n):
        return pl.ds(pl.multiple_of(n * cc, cc), cc)

    def d1_copy(job, r):
        across, apart = r // zb, r % zb
        piece = cross_out.at[job, across * zb + lax.rem(z_odd + apart, zb)]
        return send(piece, cross_in.at[job, r - 1], d1_send.at[0], d1_recv.at[job], block_peer(across, apart))

    def d1_arrival(job):
        return send(cross_in.at[job], cross_in.at[job], d1_send.at[0], d1_recv.at[job], x_peer)

    def d2_copy(n):
        return send(line_out.at[n], line_in.at[n], d2_send.at[0], d2_recv.at[n], z_peer(zb))

    def d_first(g, n, width_of):
        with scope("d_first"):
            rows = hidden[g].reshape(PAIR * gh, chunks * nc)
            values = [
                jnp.dot(rows, down_v[:, (n + i) * cc : (n + i + 1) * cc], preferred_element_type=jnp.float32)
                for i in range(width_of)
            ]
            for i, value in enumerate(values):
                job = g * columns + n + i
                value = value.reshape(PAIR * zb, tok, cc)
                own[job] = value
                cross_out[job] = value.astype(jnp.bfloat16)
                for r in range(1, PAIR * zb):
                    d1_copy(job, r).start()

    alone = columns % PAIR
    parts = [(0, alone)] * (alone > 0) + [(n, PAIR) for n in range(alone, columns, PAIR)]

    def block_sum(job):
        total = own[job, z_odd]
        d1_arrival(job).wait_recv()
        for r in range(1, PAIR * zb):
            total = total + cross_in[job, r - 1].astype(jnp.float32)
        return total

    def d_near(n):
        with scope("d_near"):
            cross_sum[n] = block_sum(n)

    def d_far(n):
        with scope("d_far"):
            line_out[n] = block_sum(n + columns).astype(jnp.bfloat16)
            d2_copy(n).start()

    def d_third(n):
        with scope("d_third"):
            mlp_out = cross_sum[n]
            d2_copy(n).wait_recv()
            mlp_out = mlp_out + line_in[n].astype(jnp.float32)
            for i in range(streams):
                value = mixed[i, :, cols(n)] + column(post[i], 0) * mlp_out
                out_ref[i, :, cols(n)] = value.astype(jnp.bfloat16)

    forward(inner)
    streams_mixed(0)
    forward(outer)
    with scope("b_wait"):
        bz_arrival(mate).wait_recv()
        bx_all(0).wait_recv()

    def sum_body(job, size):
        with scope("c1_wait"):
            c1_copy(job, size).wait_recv()
        run(c_second, job, size)

    lead = [1, BODY - 1] + [BODY] * (chunks // BODY - 1)
    even = [BODY] * (chunks // BODY)
    base = chunks / BODY + FAR_GAP
    timed = [(base - 0.01, far_wait, (0,))]
    for g, (origin, sizes) in enumerate(((0, lead), (base, even))):
        done = 0
        for size in sizes:
            job = g * chunks + done
            begin, done = origin + done / BODY, done + size
            end = origin + done / BODY
            timed += [
                (begin, c_first, (job, size)),
                (end + SUM_AT[g], sum_body, (job, size)),
                (end + HIDDEN_AT if g else base + NEAR_HIDDEN + begin / LANES, run, (c_third, job, size)),
                (end + FORWARD_AT if g else base + NEAR_FORWARD + begin / LANES, run, (c_fourth, job, size)),
            ]
    for _, stage, values in sorted(timed, key=lambda item: item[0]):
        stage(*values)

    weight_wait(2)
    for g in (1, 0):
        with scope("c4_wait"):
            c4_arrival(g).wait_recv()
        for n, count_of in parts:
            d_first(g, n, count_of)
    run(d_far, 0, columns)
    run(d_near, 0, columns)
    run(d_third, 0, columns)

    with scope("drain"):
        a_all().wait_send()
        for g in range(GROUPS):
            bx_all(g).wait_send()
        whole = [
            (rows_all.at[pl.ds(0, zs - 1)], bz_send),
            (pair_in, c1_send),
            (ring_in, c2_send),
            (hidden.at[:, pl.ds(0, ys - 1)], c3_send),
            (hidden.at[:, pl.ds(0, ys)], c4_send),
            (cross_in, d1_send),
            (line_in, d2_send),
        ]
        for ref, sem in whole:
            send(ref, ref, sem.at[0], sem.at[0], x_peer).wait_send()


def layer_scratch(zs, ys, tensors, tok, streams, logits, width, units, nc, cc):
    zb = zs // GROUPS
    gh = zb * tok
    gq = gh // ys
    chunks, columns = units // nc, width // cc
    jobs = GROUPS * columns
    f32, bf16 = jnp.float32, jnp.bfloat16
    arrays = [
        ((units, width), bf16),
        ((units, width), bf16),
        ((units, width), bf16),
        ((tok, streams, width), bf16),
        ((logits, streams, width), bf16),
        ((streams, tok, width), bf16),
        ((streams, logits, width), bf16),
        ((tok, LANES), f32),
        ((tensors - 1, tok, LANES), f32),
        ((tok, LANES), f32),
        ((tok, LANES), f32),
        ((streams, tok, LANES), f32),
        ((PAIR * zs, tok, width), bf16),
        ((streams, tok, width), f32),
        ((chunks * GROUPS, PAIR, gh, 2 * nc), f32),
        ((chunks * GROUPS, gh, 2 * nc), f32),
        ((chunks * GROUPS, ys - 1, gq, 2 * nc), bf16),
        ((chunks * GROUPS, ys - 1, gq, 2 * nc), bf16),
        ((GROUPS, PAIR * ys, gq, units), bf16),
        ((jobs, PAIR * zb, tok, cc), f32),
        ((jobs, PAIR * zb, tok, cc), bf16),
        ((jobs, PAIR * zb - 1, tok, cc), bf16),
        ((columns, tok, cc), f32),
        ((columns, tok, cc), bf16),
        ((columns, tok, cc), bf16),
    ]
    sems = [(2,), (3,)]
    for count in (1, zs, GROUPS, chunks * GROUPS, chunks * GROUPS, chunks * GROUPS * (ys - 1), GROUPS, jobs, columns):
        sems += [(1,), (count,)]
    size = sum(math.prod(shape) * jnp.dtype(kind).itemsize for shape, kind in arrays)
    return arrays, sems, size


def fused(mesh, streams, mix_weight, mix_bias, gate_weight, up_weight, down_weight):
    tok, stream_count, width = streams.shape
    units = gate_weight.shape[0]
    dps, tensors = mesh.shape["dp"], mesh.shape["tensor"]
    zs, ys = dps // PAIR, tensors // PAIR
    nc, cc = UNIT_CHUNK, COLUMN_CHUNK
    arrays, sems, _ = layer_scratch(zs, ys, tensors, tok, stream_count, mix_weight.shape[0], width, units, nc, cc)
    plan = (zs, ys, tensors, units // nc, nc, width // cc, cc, stream_count * width * tensors)
    bias = mix_bias[None, :]
    vmem = pl.BlockSpec(memory_space=pltpu.VMEM)
    hbm = pl.BlockSpec(memory_space=pl.ANY)
    out = pl.pallas_call(
        functools.partial(layer_kernel, plan),
        out_shape=pltpu.VMEM((stream_count, tok, width), jnp.bfloat16),
        in_specs=[hbm, hbm, vmem, hbm, hbm, hbm],
        out_specs=vmem,
        scratch_shapes=[pltpu.VMEM(shape, kind) for shape, kind in arrays]
        + [pltpu.SemaphoreType.DMA(shape) for shape in sems],
        compiler_params=pltpu.CompilerParams(
            collective_id=0, has_side_effects=True, vmem_limit_bytes=VMEM_BUDGET
        ),
    )(streams, mix_weight, bias, gate_weight, up_weight, down_weight)
    return out.transpose(1, 0, 2)


def fits(mesh, streams, mix_weight, gate_weight):
    tok, stream_count, width = streams.shape
    units = gate_weight.shape[0]
    dps, tensors = mesh.shape["dp"], mesh.shape["tensor"]
    if dps != PAIR * GROUPS * PAIR or tensors % PAIR or tensors < 2 * PAIR:
        return False
    zs, ys = dps // PAIR, tensors // PAIR
    if units % (BODY * UNIT_CHUNK) or width % UNIT_CHUNK or width % COLUMN_CHUNK or tok % 16 or (zs // GROUPS * tok) % (16 * ys):
        return False
    if mix_weight.shape[0] >= LANES:
        return False
    size = layer_scratch(
        zs, ys, tensors, tok, stream_count, mix_weight.shape[0], width, units, UNIT_CHUNK, COLUMN_CHUNK
    )[2]
    return size < VMEM_BUDGET * 3 // 4


def solution(mesh):
    in_specs = (
        P("dp", None, "tensor"),
        P(None, None, "tensor"),
        P(),
        P("dp", "tensor"),
        P("dp", "tensor"),
        P("dp", "tensor"),
    )
    out_specs = P("dp", None, "tensor")

    def step(streams, mix_weight, mix_bias, gate_weight, up_weight, down_weight):
        operands = (streams, mix_weight, mix_bias, gate_weight, up_weight, down_weight)
        if fits(mesh, streams, mix_weight, gate_weight):
            return fused(mesh, *operands)
        return per_device(*operands)

    return jax.shard_map(step, mesh=mesh, in_specs=in_specs, out_specs=out_specs, check_vma=False)
```
